256 devices in a mesh: row: 16 (over y_hi, z), col: 16 (over x, y_lo, core).
Axes of the slice: x: 4, y: 4 (y_hi: 2, y_lo: 2; y = y_hi * 2 + y_lo), z: 8, core: 2. Of those that a mesh axis runs over, the one named last changes fastest.
Arguments:
- fields: float32 [1, 4, 256, 256, 256], P(None, None, 'row', 'col'), may hold values from -6 to 6
- cotangent: float32 [1, 4, 256, 256, 256], P(None, None, 'row', 'col'), may hold values from -6 to 6
- spec_weights: float32 [2, 4, 4, 16, 16, 16], replicated, may hold values from -96 to 96
- point_weights: float32 [4, 4], replicated, may hold values from -3 to 3
- bias: float32 [4], replicated, may hold values from -3 to 3
Outputs:
- grad_fields: float32 [1, 4, 256, 256, 256], P(None, None, 'row', 'col')
- grad_spectral: float32 [2, 4, 4, 16, 16, 16], replicated
The draws below stay inside these ranges and needn't reach their ends.
All inputs are finite; a program needn't handle non-finite values.
Results may differ from the reference program's by a relative error of at most 0.00011.
Values sent between devices are 32-bit elements; how exact they have to be, the bound alone decides.
No kernel may reach another device: no remote copies, remote signals or barrier semaphores. Data moves between devices by JAX's collectives and lax.ppermute only.
A program may use at most 64 MiB of HBM per device.

```python
import jax
import jax.numpy as jnp
from jax import lax

B = 1
C = 4
NX = 256
NY = 256
NZ = 256
MX = 16
MY = 16
MZ = 16


def block_levels(rng, shape, shards, smallest, top_value):
    factor_of, own = 1.0, jax.random.fold_in(rng, 6)
    for axis_at, parts in shards:
        draws = jnp.exp(jax.random.uniform(jax.random.fold_in(own, axis_at), (parts,), jnp.float32, smallest / len(shards), top_value / len(shards)))
        factor_of = factor_of * jnp.repeat(draws, shape[axis_at] // parts).reshape([-1 if axis == axis_at else 1 for axis in range(len(shape))])
    return factor_of


def gaussian(rng, extent, scale, most, cuts=(), kind=jnp.bfloat16):
    loudness = block_levels(rng, extent, cuts, -0.22, 0.18) if cuts else 1.0
    entries = jax.random.normal(rng, extent, jnp.float32) * scale * loudness
    return jnp.minimum(jnp.maximum(entries, -most), most).astype(kind)


def setup_inputs(seed: int = 0) -> dict:
    splits = jax.random.split(jax.random.key(seed), 6)
    return {
        "fields": gaussian(splits[0], (B, C, NY, NZ, NX), 1.0, 6.0, ((2, 16), (3, 16)), jnp.float32),
        "cotangent": gaussian(splits[1], (B, C, NY, NZ, NX), 1.0, 6.0, ((2, 16), (3, 16)), jnp.float32),
        "spec_weights": gaussian(splits[2], (2, C, C, MX, MY, MZ), ((NX * NY * NZ / (4.0 * C * MX * MY * MZ)) ** 0.5), 96.0, (), jnp.float32),
        "point_weights": gaussian(splits[3], (C, C), C ** -0.5, 3.0, (), jnp.float32),
        "bias": gaussian(splits[4], (C,), 0.5, 3.0, (), jnp.float32),
    }


def crop(spectrum):
    spectrum = spectrum[..., :MX]
    spectrum = jnp.concatenate([spectrum[..., :MY // 2, :, :], spectrum[..., NY - MY // 2:, :, :]], axis=-3)
    spectrum = jnp.concatenate([spectrum[..., :MZ // 2, :], spectrum[..., NZ - MZ // 2:, :]], axis=-2)
    return spectrum

def expand(modes):
    lead = modes.shape[:2]
    modes = jnp.pad(modes, [(0, 0), (0, 0), (0, 0), (0, 0), (0, NX // 2 + 1 - MX)])
    width_x = modes.shape[4]
    zeros_z = jnp.zeros(lead + (MY, NZ - MZ, width_x), modes.dtype)
    modes = jnp.concatenate([modes[..., :MZ // 2, :], zeros_z, modes[..., MZ // 2:, :]], axis=-2)
    zeros_y = jnp.zeros(lead + (NY - MY, NZ, width_x), modes.dtype)
    modes = jnp.concatenate([modes[..., :MY // 2, :, :], zeros_y, modes[..., MY // 2:, :, :]], axis=-3)
    return modes

def spectral(fields, spec_weights):
    spectrum = crop(jnp.fft.rfftn(fields, axes=(2, 3, 4)))
    weights = spec_weights[0] + 1j * spec_weights[1]
    mixed_modes = jnp.einsum('biqrp,iopqr->boqrp', spectrum, weights, precision=lax.Precision.HIGHEST)
    return jnp.fft.irfftn(expand(mixed_modes), s=(NY, NZ, NX), axes=(2, 3, 4))

def reference(fields, cotangent, spec_weights, point_weights, bias):

    def forward(field_in, weight_in):
        local_term = jnp.einsum('bcyzx,co->boyzx', field_in, point_weights, precision=lax.Precision.HIGHEST)
        pre_activation = spectral(field_in, weight_in) + local_term + bias[None, :, None, None, None]
        return jax.nn.gelu(pre_activation, approximate=False)
    output, pullback = jax.vjp(forward, fields, spec_weights)
    grad_fields, grad_spectral = pullback(cotangent.astype(output.dtype))
    return (grad_fields, grad_spectral)
```

```python
import functools
import math

import jax
import jax.numpy as jnp
import numpy as np
from jax import lax
from jax.experimental import pallas as pl
from jax.experimental.pallas import tpu as pltpu
from jax.sharding import PartitionSpec as P

C = 4
N = 256
K = 16
LOCAL = 16
CELLS = LOCAL * LOCAL
MODES = K * K
ROWS = 2 * C * K

VMEM = pl.BlockSpec(memory_space=pltpu.VMEM)
SMEM = pl.BlockSpec(memory_space=pltpu.SMEM)
NT = (((1,), (1,)), ((), ()))
NN = (((1,), (0,)), ((), ()))
TN = (((0,), (0,)), ((), ()))


def two_parts(table):
    high = np.asarray(table, jnp.bfloat16)
    low = np.asarray(table - np.asarray(high, np.float64), jnp.bfloat16)
    return np.stack([high, low])


def signed_waves():
    index = np.arange(K)
    return np.where(index < K // 2, index, index - K)


def tables():
    angle = 2.0 * np.pi / N * (np.arange(K)[:, None] * np.arange(N)[None, :] % N)
    forward_x = np.concatenate([np.cos(angle), -np.sin(angle)], 0)
    weighting = np.where(np.arange(K) == 0, 1.0, 2.0)[:, None] / float(N) ** 3
    inverse_x = np.concatenate([np.cos(angle) * weighting, -np.sin(angle) * weighting], 0)
    one = np.arange(LOCAL)[:, None] * signed_waves()[None, :]
    both = one[:, None, :, None] + one[None, :, None, :]
    angle = 2.0 * np.pi / N * (both.reshape(CELLS, MODES) % N)
    plane = np.concatenate([np.cos(angle), -np.sin(angle)], 1)
    return two_parts(forward_x), two_parts(inverse_x), two_parts(plane)


def split(value):
    high = value.astype(jnp.bfloat16)
    low = (value - high.astype(jnp.float32)).astype(jnp.bfloat16)
    return high, low


def dot3(left, right, dims):
    dot = functools.partial(
        lax.dot_general, dimension_numbers=dims, preferred_element_type=jnp.float32
    )
    return dot(left[0], right[0]) + (dot(left[0], right[1]) + dot(left[1], right[0]))


def analyse(channel, phase, forward_x, plane):
    real, imag = [], []
    for c in range(C):
        along_x = dot3(forward_x, split(channel(c)), NT)
        real.append(along_x[:K])
        imag.append(along_x[K:])
    both = dot3(split(jnp.concatenate(real + imag, 0)), plane, NN)
    half = ROWS // 2
    part_re = both[:half, :MODES] - both[half:, MODES:]
    part_im = both[:half, MODES:] + both[half:, :MODES]
    cosine, sine = phase[0:1, :], phase[1:2, :]
    return part_re * cosine - part_im * sine, part_re * sine + part_im * cosine


def synthesise(modes_re, modes_im, phase, inverse_x, plane):
    cosine, sine = phase[0:1, :], phase[1:2, :]
    here_re = modes_re * cosine + modes_im * sine
    here_im = modes_im * cosine - modes_re * sine
    left = jnp.concatenate(
        [jnp.concatenate([here_re, here_im], 1), jnp.concatenate([here_im, -here_re], 1)], 0
    )
    lines = dot3(split(left), plane, NT)
    half = ROWS // 2
    out = []
    for c in range(C):
        pair = jnp.concatenate([lines[c * K : (c + 1) * K], lines[half + c * K :][:K]], 0)
        out.append(dot3(split(pair), inverse_x, TN))
    return out


def parts(ref):
    return ref[0], ref[1]


def analysis_kernel(fields, phase, forward_x, plane, out):
    result = analyse(lambda c: fields[c], phase[...], parts(forward_x), parts(plane))
    out[: ROWS // 2] = result[0]
    out[ROWS // 2 :] = result[1]


def spread_kernel(pieces, out):
    total = jnp.sum(pieces[...], axis=0)
    out[...] = jnp.broadcast_to(total[None], out.shape)


def take(ref, t, c):
    start = (t * C + c) * K
    return ref[start : start + K]


def forward_kernel(
    modes, weights, fields, cotangent, point, bias, phase, forward_x, inverse_x, plane, up, out
):
    mixed_re, mixed_im = [], []
    for o in range(C):
        re = im = None
        for i in range(C):
            a, b = take(modes, 0, i), take(modes, 1, i)
            w, v = weights[0, i, o], weights[1, i, o]
            re = a * w - b * v if re is None else re + (a * w - b * v)
            im = a * v + b * w if im is None else im + (a * v + b * w)
        mixed_re.append(re)
        mixed_im.append(im)
    term = synthesise(
        jnp.concatenate(mixed_re, 0),
        jnp.concatenate(mixed_im, 0),
        phase[...],
        parts(inverse_x),
        parts(plane),
    )
    for o in range(C):
        pre = term[o] + bias[o]
        for i in range(C):
            pre = pre + point[i, o] * fields[i]
        slope = 0.5 * (1.0 + lax.erf(pre * math.sqrt(0.5))) + pre * jnp.exp(
            -0.5 * pre * pre
        ) * (1.0 / math.sqrt(2.0 * math.pi))
        up[o] = cotangent[o] * slope
    result = analyse(lambda c: up[c], phase[...], parts(forward_x), parts(plane))
    out[: ROWS // 2] = result[0]
    out[ROWS // 2 :] = result[1]


def backward_kernel(
    modes, back, weights, up, point, phase, inverse_x, plane, factor, grad_fields, grad_spectral
):
    adjoint_re, adjoint_im = [], []
    for i in range(C):
        re = im = None
        for o in range(C):
            a, b = take(back, 0, o), take(back, 1, o)
            w, v = weights[0, i, o], weights[1, i, o]
            re = a * w + b * v if re is None else re + (a * w + b * v)
            im = b * w - a * v if im is None else im + (b * w - a * v)
        adjoint_re.append(re)
        adjoint_im.append(im)
    term = synthesise(
        jnp.concatenate(adjoint_re, 0),
        jnp.concatenate(adjoint_im, 0),
        phase[...],
        parts(inverse_x),
        parts(plane),
    )
    for i in range(C):
        total = term[i]
        for o in range(C):
            total = total + point[i, o] * up[o]
        grad_fields[i] = total
    for o in range(C):
        a, b = take(back, 0, o) * factor[...], take(back, 1, o) * factor[...]
        for i in range(C):
            u, w = take(modes, 0, i), take(modes, 1, i)
            grad_spectral[0, i, o] = u * a + w * b
            grad_spectral[1, i, o] = u * b - w * a


def position_phase():
    lane = jnp.arange(MODES, dtype=jnp.int32)
    steps = (lane // K) * lax.axis_index("row") + (lane % K) * lax.axis_index("col")
    angle = (steps % K).astype(jnp.float32) * (2.0 * math.pi / K)
    return jnp.stack([jnp.cos(angle), -jnp.sin(angle)], 0)


def swap(pieces, axis):
    return lax.all_to_all(pieces, axis, 0, 0, tiled=True)


def total_modes(partial):
    shape = jax.ShapeDtypeStruct((K, ROWS // K, MODES), jnp.float32)
    spread = pl.pallas_call(spread_kernel, out_shape=shape, in_specs=[VMEM], out_specs=VMEM)
    pieces = swap(partial.reshape(shape.shape), "col")
    pieces = swap(spread(pieces), "row")
    pieces = swap(spread(pieces), "col")
    return pieces.reshape(ROWS, MODES)


def per_device(fields, cotangent, spec_weights, point_weights, bias):
    forward_x, inverse_x, plane = [jnp.asarray(t) for t in tables()]
    factor = np.where(np.arange(K) == 0, 1.0, 2.0) / float(N) ** 3
    factor = jnp.asarray(np.broadcast_to(factor[:, None], (K, MODES)), jnp.float32)
    cells = (C, CELLS, N)
    shape = fields.shape
    fields = fields.reshape(cells)
    cotangent = cotangent.reshape(cells)
    weights = spec_weights.reshape(2, C, C, K, MODES)
    phase = position_phase()
    float_of = functools.partial(jax.ShapeDtypeStruct, dtype=jnp.float32)
    partial = pl.pallas_call(
        analysis_kernel,
        out_shape=float_of((ROWS, MODES)),
        in_specs=[VMEM] * 4,
        out_specs=VMEM,
    )(fields, phase, forward_x, plane)
    modes = total_modes(partial)
    upstream, partial = pl.pallas_call(
        forward_kernel,
        out_shape=(float_of(cells), float_of((ROWS, MODES))),
        in_specs=[VMEM] * 4 + [SMEM] * 2 + [VMEM] * 4,
        out_specs=(VMEM, VMEM),
    )(
        modes, weights, fields, cotangent, point_weights, bias, phase, forward_x, inverse_x, plane
    )
    back = total_modes(partial)
    grad_fields, grad_spectral = pl.pallas_call(
        backward_kernel,
        out_shape=(float_of(cells), float_of((2, C, C, K, MODES))),
        in_specs=[VMEM] * 4 + [SMEM] + [VMEM] * 4,
        out_specs=(VMEM, VMEM),
    )(modes, back, weights, upstream, point_weights, phase, inverse_x, plane, factor)
    return grad_fields.reshape(shape), grad_spectral.reshape(spec_weights.shape)


def solution(mesh):
    placed = P(None, None, "row", "col", None)
    return jax.shard_map(
        per_device,
        mesh=mesh,
        in_specs=(placed, placed, P(), P(), P()),
        out_specs=(placed, P()),
        check_vma=False,
    )
```

```python
import functools
import math

import jax
import jax.numpy as jnp
import numpy as np
from jax import lax
from jax.experimental import pallas as pl
from jax.experimental.pallas import tpu as pltpu
from jax.sharding import PartitionSpec as P

C = 4
N = 256
K = 16
LOCAL = 16
CELLS = LOCAL * LOCAL
MODES = K * K
ROWS = 2 * C * K

VMEM = pl.BlockSpec(memory_space=pltpu.VMEM)
SMEM = pl.BlockSpec(memory_space=pltpu.SMEM)
PARAMS = pltpu.CompilerParams(vmem_limit_bytes=24 << 20)
NT = (((1,), (1,)), ((), ()))
NN = (((1,), (0,)), ((), ()))
TN = (((0,), (0,)), ((), ()))


def two_parts(table):
    high = np.asarray(table, jnp.bfloat16)
    low = np.asarray(table - np.asarray(high, np.float64), jnp.bfloat16)
    return np.stack([high, low])


def signed_waves():
    index = np.arange(K)
    return np.where(index < K // 2, index, index - K)


def tables():
    angle = 2.0 * np.pi / N * (np.arange(K)[:, None] * np.arange(N)[None, :] % N)
    forward_x = np.concatenate([np.cos(angle), -np.sin(angle)], 0)
    weighting = np.where(np.arange(K) == 0, 1.0, 2.0)[:, None] / float(N) ** 3
    inverse_x = np.concatenate([np.cos(angle) * weighting, -np.sin(angle) * weighting], 0)
    one = np.arange(LOCAL)[:, None] * signed_waves()[None, :]
    both = one[:, None, :, None] + one[None, :, None, :]
    angle = 2.0 * np.pi / N * (both.reshape(CELLS, MODES) % N)
    plane = np.concatenate([np.cos(angle), -np.sin(angle)], 1)
    return two_parts(forward_x), two_parts(inverse_x), two_parts(plane)


def split(value):
    high = value.astype(jnp.bfloat16)
    low = (value - high.astype(jnp.float32)).astype(jnp.bfloat16)
    return high, low


def dot3(left, right, dims):
    dot = functools.partial(
        lax.dot_general, dimension_numbers=dims, preferred_element_type=jnp.float32
    )
    return dot(left[0], right[0]) + (dot(left[0], right[1]) + dot(left[1], right[0]))


def analyse(channel, phase, forward_x, plane):
    real, imag = [], []
    for c in range(C):
        along_x = dot3(forward_x, split(channel(c)), NT)
        real.append(along_x[:K])
        imag.append(along_x[K:])
    both = dot3(split(jnp.concatenate(real + imag, 0)), plane, NN)
    half = ROWS // 2
    part_re = both[:half, :MODES] - both[half:, MODES:]
    part_im = both[:half, MODES:] + both[half:, :MODES]
    cosine, sine = phase[0:1, :], phase[1:2, :]
    return part_re * cosine - part_im * sine, part_re * sine + part_im * cosine


def synthesise(modes_re, modes_im, phase, inverse_x, plane):
    cosine, sine = phase[0:1, :], phase[1:2, :]
    here_re = modes_re * cosine + modes_im * sine
    here_im = modes_im * cosine - modes_re * sine
    left = jnp.concatenate(
        [jnp.concatenate([here_re, here_im], 1), jnp.concatenate([here_im, -here_re], 1)], 0
    )
    lines = dot3(split(left), plane, NT)
    half = ROWS // 2
    out = []
    for c in range(C):
        pair = jnp.concatenate([lines[c * K : (c + 1) * K], lines[half + c * K :][:K]], 0)
        out.append(dot3(split(pair), inverse_x, TN))
    return out


def parts(ref):
    return ref[0], ref[1]


def analysis_kernel(fields, phase, forward_x, plane, out):
    result = analyse(lambda c: fields[c], phase[...], parts(forward_x), parts(plane))
    out[: ROWS // 2] = result[0]
    out[ROWS // 2 :] = result[1]


def spread_kernel(pieces, out):
    total = jnp.sum(pieces[...], axis=0)
    out[...] = jnp.broadcast_to(total[None], out.shape)


def take(ref, t, c):
    start = (t * C + c) * K
    return ref[start : start + K]


def forward_kernel(
    modes, weights, fields, cotangent, point, bias, phase, forward_x, inverse_x, plane, up, out
):
    mixed_re, mixed_im = [], []
    for o in range(C):
        re = im = None
        for i in range(C):
            a, b = take(modes, 0, i), take(modes, 1, i)
            w, v = weights[0, i, o], weights[1, i, o]
            re = a * w - b * v if re is None else re + (a * w - b * v)
            im = a * v + b * w if im is None else im + (a * v + b * w)
        mixed_re.append(re)
        mixed_im.append(im)
    term = synthesise(
        jnp.concatenate(mixed_re, 0),
        jnp.concatenate(mixed_im, 0),
        phase[...],
        parts(inverse_x),
        parts(plane),
    )
    for o in range(C):
        pre = term[o] + bias[o]
        for i in range(C):
            pre = pre + point[i, o] * fields[i]
        slope = 0.5 * (1.0 + lax.erf(pre * math.sqrt(0.5))) + pre * jnp.exp(
            -0.5 * pre * pre
        ) * (1.0 / math.sqrt(2.0 * math.pi))
        up[o] = cotangent[o] * slope
    result = analyse(lambda c: up[c], phase[...], parts(forward_x), parts(plane))
    out[: ROWS // 2] = result[0]
    out[ROWS // 2 :] = result[1]


def backward_kernel(
    modes, back, weights, up, point, phase, inverse_x, plane, factor, grad_fields, grad_spectral
):
    adjoint_re, adjoint_im = [], []
    for i in range(C):
        re = im = None
        for o in range(C):
            a, b = take(back, 0, o), take(back, 1, o)
            w, v = weights[0, i, o], weights[1, i, o]
            re = a * w + b * v if re is None else re + (a * w + b * v)
            im = b * w - a * v if im is None else im + (b * w - a * v)
        adjoint_re.append(re)
        adjoint_im.append(im)
    term = synthesise(
        jnp.concatenate(adjoint_re, 0),
        jnp.concatenate(adjoint_im, 0),
        phase[...],
        parts(inverse_x),
        parts(plane),
    )
    for i in range(C):
        total = term[i]
        for o in range(C):
            total = total + point[i, o] * up[o]
        grad_fields[i] = total
    for o in range(C):
        a, b = take(back, 0, o) * factor[...], take(back, 1, o) * factor[...]
        for i in range(C):
            u, w = take(modes, 0, i), take(modes, 1, i)
            grad_spectral[0, i, o] = u * a + w * b
            grad_spectral[1, i, o] = u * b - w * a


def position_phase():
    lane = jnp.arange(MODES, dtype=jnp.int32)
    steps = (lane // K) * lax.axis_index("row") + (lane % K) * lax.axis_index("col")
    angle = (steps % K).astype(jnp.float32) * (2.0 * math.pi / K)
    return jnp.stack([jnp.cos(angle), -jnp.sin(angle)], 0)


def near(value):
    return pltpu.with_memory_space_constraint(value, pltpu.VMEM)


def near_out(shape):
    return pltpu.VMEM(shape, jnp.float32)


def swap(pieces, axis):
    return lax.all_to_all(pieces, axis, 0, 0, tiled=True)


def total_modes(partial):
    shape = (K, ROWS // K, MODES)
    spread = pl.pallas_call(
        spread_kernel,
        out_shape=near_out(shape),
        in_specs=[VMEM],
        out_specs=VMEM,
        compiler_params=PARAMS,
    )
    pieces = swap(partial.reshape(shape), "col")
    pieces = swap(spread(near(pieces)), "row")
    pieces = swap(spread(near(pieces)), "col")
    return near(pieces.reshape(ROWS, MODES))


def per_device(fields, cotangent, spec_weights, point_weights, bias):
    forward_x, inverse_x, plane = [jnp.asarray(t) for t in tables()]
    factor = np.where(np.arange(K) == 0, 1.0, 2.0) / float(N) ** 3
    factor = jnp.asarray(np.broadcast_to(factor[:, None], (K, MODES)), jnp.float32)
    cells = (C, CELLS, N)
    shape = fields.shape
    fields = fields.reshape(cells)
    cotangent = cotangent.reshape(cells)
    weights = spec_weights.reshape(2, C, C, K, MODES)
    phase = position_phase()
    fields, cotangent, weights, phase = [near(v) for v in (fields, cotangent, weights, phase)]
    forward_x, inverse_x, plane = [near(v) for v in (forward_x, inverse_x, plane)]
    float_of = functools.partial(jax.ShapeDtypeStruct, dtype=jnp.float32)
    partial = pl.pallas_call(
        analysis_kernel,
        out_shape=near_out((ROWS, MODES)),
        in_specs=[VMEM] * 4,
        out_specs=VMEM,
        compiler_params=PARAMS,
    )(fields, phase, forward_x, plane)
    modes = total_modes(partial)
    upstream, partial = pl.pallas_call(
        forward_kernel,
        out_shape=(near_out(cells), near_out((ROWS, MODES))),
        in_specs=[VMEM] * 4 + [SMEM] * 2 + [VMEM] * 4,
        out_specs=(VMEM, VMEM),
        compiler_params=PARAMS,
    )(
        modes, weights, fields, cotangent, point_weights, bias, phase, forward_x, inverse_x, plane
    )
    back = total_modes(partial)
    grad_fields, grad_spectral = pl.pallas_call(
        backward_kernel,
        out_shape=(float_of(cells), float_of((2, C, C, K, MODES))),
        in_specs=[VMEM] * 4 + [SMEM] + [VMEM] * 4,
        out_specs=(VMEM, VMEM),
        compiler_params=PARAMS,
    )(modes, back, weights, near(upstream), point_weights, phase, inverse_x, plane, factor)
    return grad_fields.reshape(shape), grad_spectral.reshape(spec_weights.shape)


def solution(mesh):
    placed = P(None, None, "row", "col", None)
    return jax.shard_map(
        per_device,
        mesh=mesh,
        in_specs=(placed, placed, P(), P(), P()),
        out_specs=(placed, P()),
        check_vma=False,
    )
```

```python
import functools
import math

import jax
import jax.numpy as jnp
import numpy as np
from jax import lax
from jax.experimental import pallas as pl
from jax.experimental.pallas import tpu as pltpu
from jax.sharding import PartitionSpec as P

C = 4
N = 256
K = 16
LOCAL = 16
CELLS = LOCAL * LOCAL
MODES = K * K
ROWS = 2 * C * K

VMEM = pl.BlockSpec(memory_space=pltpu.VMEM)
HBM = pl.BlockSpec(memory_space=pltpu.HBM)
SMEM = pl.BlockSpec(memory_space=pltpu.SMEM)
PARAMS = pltpu.CompilerParams(vmem_limit_bytes=24 << 20)
NT = (((1,), (1,)), ((), ()))
NN = (((1,), (0,)), ((), ()))
TN = (((0,), (0,)), ((), ()))


def two_parts(table):
    high = np.asarray(table, jnp.bfloat16)
    low = np.asarray(table - np.asarray(high, np.float64), jnp.bfloat16)
    return np.stack([high, low])


def signed_waves():
    index = np.arange(K)
    return np.where(index < K // 2, index, index - K)


def tables():
    angle = 2.0 * np.pi / N * (np.arange(K)[:, None] * np.arange(N)[None, :] % N)
    forward_x = np.concatenate([np.cos(angle), -np.sin(angle)], 0)
    weighting = np.where(np.arange(K) == 0, 1.0, 2.0)[:, None] / float(N) ** 3
    inverse_x = np.concatenate([np.cos(angle) * weighting, -np.sin(angle) * weighting], 0)
    one = np.arange(LOCAL)[:, None] * signed_waves()[None, :]
    both = one[:, None, :, None] + one[None, :, None, :]
    angle = 2.0 * np.pi / N * (both.reshape(CELLS, MODES) % N)
    plane = np.concatenate([np.cos(angle), -np.sin(angle)], 1)
    return two_parts(forward_x), two_parts(inverse_x), two_parts(plane)


def split(value):
    high = value.astype(jnp.bfloat16)
    low = (value - high.astype(jnp.float32)).astype(jnp.bfloat16)
    return high, low


def dot3(left, right, dims):
    dot = functools.partial(
        lax.dot_general, dimension_numbers=dims, preferred_element_type=jnp.float32
    )
    return dot(left[0], right[0]) + (dot(left[0], right[1]) + dot(left[1], right[0]))


def analyse(channel, phase, forward_x, plane, out, ready=None):
    real, imag = [], []
    for c in range(C):
        along_x = dot3(forward_x, split(channel(c)), NT)
        real.append(along_x[:K])
        imag.append(along_x[K:])
    if ready is not None:
        ready()
    both = dot3(split(jnp.concatenate(real + imag, 0)), parts(plane), NN)
    half = ROWS // 2
    part_re = both[:half, :MODES] - both[half:, MODES:]
    part_im = both[:half, MODES:] + both[half:, :MODES]
    cosine, sine = phase[0:1, :], phase[1:2, :]
    for t, part in enumerate(
        (part_re * cosine - part_im * sine, part_re * sine + part_im * cosine)
    ):
        for c in range(C):
            out[:, t * C + c, :] = part[c * K : (c + 1) * K]


def synthesise(modes_re, modes_im, phase, inverse_x, plane):
    cosine, sine = phase[0:1, :], phase[1:2, :]
    here_re = modes_re * cosine + modes_im * sine
    here_im = modes_im * cosine - modes_re * sine
    left = jnp.concatenate(
        [jnp.concatenate([here_re, here_im], 1), jnp.concatenate([here_im, -here_re], 1)], 0
    )
    lines = dot3(split(left), plane, NT)
    half = ROWS // 2
    out = []
    for c in range(C):
        pair = jnp.concatenate([lines[c * K : (c + 1) * K], lines[half + c * K :][:K]], 0)
        out.append(dot3(split(pair), inverse_x, TN))
    return out


def parts(ref):
    return ref[0], ref[1]


def own_wave():
    flip = 2 * (lax.axis_index("row") // (K // 2))
    return jnp.bitwise_xor(lax.axis_index("col"), flip)


def analysis_kernel(
    fields, forward_x, plane, stored, phase, out, cells, weights, lines, square, slab, arrived
):
    table = pltpu.make_async_copy(forward_x, lines, arrived.at[C])
    table.start()
    copies = [
        pltpu.make_async_copy(fields.at[c], cells.at[c], arrived.at[c]) for c in range(C)
    ]
    for copy in copies:
        copy.start()
    second = pltpu.make_async_copy(plane, square, arrived.at[C + 1])
    second.start()
    third = pltpu.make_async_copy(stored.at[:, own_wave()], slab, arrived.at[C + 2])
    third.start()
    table.wait()

    def channel(c):
        copies[c].wait()
        return cells[c]

    analyse(channel, phase[...], parts(lines), square, out, second.wait)
    third.wait()
    weights[...] = jnp.concatenate([slab[:, q, :] for q in range(K)], 1)


def spread_kernel(pieces, out):
    total = jnp.sum(pieces[...], axis=0)
    out[...] = jnp.broadcast_to(total[None], out.shape)


def forward_mix_kernel(pieces, weights, out):
    total = jnp.sum(pieces[...], axis=0)
    re = im = 0.0
    for i in range(C):
        a, b = total[i : i + 1], total[C + i : C + i + 1]
        w, v = weights[i * C : (i + 1) * C], weights[C * C + i * C :][:C]
        re = re + (a * w - b * v)
        im = im + (a * v + b * w)
    both = jnp.concatenate([re, im, total], 0)
    out[...] = jnp.broadcast_to(both[None], out.shape)


def backward_mix_kernel(pieces, weights, out):
    total = jnp.sum(pieces[...], axis=0)
    re = im = 0.0
    for o in range(C):
        a, b = total[o : o + 1], total[C + o : C + o + 1]
        w, v = [
            jnp.concatenate([weights[pl.ds((t * C + i) * C + o, 1), :] for i in range(C)], 0)
            for t in range(2)
        ]
        re = re + (a * w + b * v)
        im = im + (b * w - a * v)
    both = jnp.concatenate([re, im, total], 0)
    out[...] = jnp.broadcast_to(both[None], out.shape)


def take(ref, row):
    return ref[:, row, :]


def take_mixed(ref):
    return [
        jnp.concatenate([take(ref, t * C + c) for c in range(C)], 0) for t in range(2)
    ]


def forward_kernel(
    modes, fields, cotangent, point, bias, phase, forward_x, inverse_x, plane, up, out
):
    term = synthesise(*take_mixed(modes), phase[...], parts(inverse_x), parts(plane))
    for o in range(C):
        pre = term[o] + bias[o]
        for i in range(C):
            pre = pre + point[i, o] * fields[i]
        slope = 0.5 * (1.0 + lax.erf(pre * math.sqrt(0.5))) + pre * jnp.exp(
            -0.5 * pre * pre
        ) * (1.0 / math.sqrt(2.0 * math.pi))
        up[o] = cotangent[o] * slope
    analyse(lambda c: up[c], phase[...], parts(forward_x), plane, out)


def backward_kernel(
    modes,
    back,
    up,
    point,
    phase,
    inverse_x,
    plane,
    factor,
    grad_fields,
    grad_spectral,
    cells,
    stored,
    sent,
):
    copies = []

    def send(source, target):
        copies.append(pltpu.make_async_copy(source, target, sent.at[len(copies)]))
        copies[-1].start()

    scaled = [
        [take(back, (2 + t) * C + o) * factor[...] for t in range(2)] for o in range(C)
    ]
    for i in range(C):
        u, w = take(modes, 2 * C + i), take(modes, 3 * C + i)
        for o in range(C):
            a, b = scaled[o]
            for t, value in enumerate((u * a + w * b, u * b - w * a)):
                for q in range(K):
                    stored[t, i, o, :, q, :] = value[:, q * K : (q + 1) * K]
        for t in range(2):
            send(stored.at[t, i], grad_spectral.at[t, i])
    term = synthesise(*take_mixed(back), phase[...], parts(inverse_x), parts(plane))
    for i in range(C):
        total = term[i]
        for o in range(C):
            total = total + point[i, o] * up[o]
        cells[i] = total
        send(cells.at[i], grad_fields.at[i])
    for copy in copies:
        copy.wait()


def position_phase():
    lane = jnp.arange(MODES, dtype=jnp.int32)
    steps = (lane // K) * lax.axis_index("row") + (lane % K) * lax.axis_index("col")
    angle = (steps % K).astype(jnp.float32) * (2.0 * math.pi / K)
    return jnp.stack([jnp.cos(angle), -jnp.sin(angle)], 0)


def near(value):
    return pltpu.with_memory_space_constraint(value, pltpu.VMEM)


def far(value):
    return pltpu.with_memory_space_constraint(value, pltpu.HBM)


def near_out(shape):
    return pltpu.VMEM(shape, jnp.float32)


def groups():
    index = np.arange(256).reshape(2, 8, 4, 2, 2)
    index[1] = index[1, :, :, ::-1]
    index = index.reshape(K, K)
    return index.tolist(), index.T.tolist()


def swap(pieces, members):
    return lax.all_to_all(
        pieces, ("row", "col"), 0, 0, tiled=True, axis_index_groups=members
    )


def call(kernel, out_shape, in_specs, scratch_shapes=()):
    where = [VMEM if not isinstance(o, jax.ShapeDtypeStruct) else HBM for o in out_shape]
    return pl.pallas_call(
        kernel,
        out_shape=tuple(out_shape),
        in_specs=in_specs,
        out_specs=tuple(where),
        scratch_shapes=scratch_shapes,
        compiler_params=PARAMS,
    )


def summed_modes(partial, weights, mix_kernel):
    shape = (K, 2 * C, MODES)
    near_by, alike = groups()
    pieces = near(swap(partial, near_by))
    (pieces,) = call(spread_kernel, [near_out(shape)], [VMEM])(pieces)
    pieces = near(swap(pieces, alike))
    shape = (K, 4 * C, MODES)
    (pieces,) = call(mix_kernel, [near_out(shape)], [VMEM] * 2)(pieces, weights)
    return near(swap(pieces, near_by))


def per_device(fields, cotangent, spec_weights, point_weights, bias):
    forward_x, inverse_x, plane = [jnp.asarray(t) for t in tables()]
    factor = np.where(np.arange(K) == 0, 1.0, 2.0) / float(N) ** 3
    factor = jnp.asarray(np.broadcast_to(factor[:, None], (K, MODES)), jnp.float32)
    shape = fields.shape
    cells = (C, CELLS, N)
    phase = near(position_phase())
    partial, fields, weights = call(
        analysis_kernel,
        [near_out((K, 2 * C, MODES)), near_out(cells), near_out((2 * C * C, MODES))],
        [HBM] * 4 + [VMEM],
        [
            pltpu.VMEM((2, 2 * K, N), jnp.bfloat16),
            pltpu.VMEM((2, CELLS, 2 * MODES), jnp.bfloat16),
            pltpu.VMEM((2 * C * C, K, K), jnp.float32),
            pltpu.SemaphoreType.DMA((C + 3,)),
        ],
    )(
        far(fields.reshape(cells)),
        far(forward_x),
        far(plane),
        far(spec_weights.reshape(2 * C * C, K, K, K)),
        phase,
    )
    weights = near(weights)
    forward_x, inverse_x, plane = [near(v) for v in (forward_x, inverse_x, plane)]
    modes = summed_modes(partial, weights, forward_mix_kernel)
    upstream, partial = call(
        forward_kernel,
        [near_out(cells), near_out((K, 2 * C, MODES))],
        [VMEM] * 3 + [SMEM] * 2 + [VMEM] * 4,
    )(
        modes,
        near(fields),
        near(cotangent.reshape(cells)),
        point_weights,
        bias,
        phase,
        forward_x,
        inverse_x,
        plane,
    )
    back = summed_modes(partial, weights, backward_mix_kernel)
    grad_fields, grad_spectral = call(
        backward_kernel,
        [
            jax.ShapeDtypeStruct(cells, jnp.float32),
            jax.ShapeDtypeStruct((2, C, C, K, K, K), jnp.float32),
        ],
        [VMEM] * 3 + [SMEM] + [VMEM] * 4,
        [
            pltpu.VMEM(cells, jnp.float32),
            pltpu.VMEM((2, C, C, K, K, K), jnp.float32),
            pltpu.SemaphoreType.DMA((3 * C,)),
        ],
    )(
        modes,
        back,
        near(upstream),
        point_weights,
        phase,
        inverse_x,
        plane,
        near(factor),
    )
    return grad_fields.reshape(shape), grad_spectral


def solution(mesh):
    placed = P(None, None, "row", "col", None)
    return jax.shard_map(
        per_device,
        mesh=mesh,
        in_specs=(placed, placed, P(), P(), P()),
        out_specs=(placed, P()),
        check_vma=False,
    )
```

```python
import functools
import math

import jax
import jax.numpy as jnp
import numpy as np
from jax import lax
from jax.experimental import pallas as pl
from jax.experimental.pallas import tpu as pltpu
from jax.sharding import PartitionSpec as P

C = 4
N = 256
K = 16
LOCAL = 16
CELLS = LOCAL * LOCAL
MODES = K * K
ROWS = 2 * C * K

VMEM = pl.BlockSpec(memory_space=pltpu.VMEM)
HBM = pl.BlockSpec(memory_space=pltpu.HBM)
SMEM = pl.BlockSpec(memory_space=pltpu.SMEM)
PARAMS = pltpu.CompilerParams(vmem_limit_bytes=24 << 20)
NT = (((1,), (1,)), ((), ()))
NN = (((1,), (0,)), ((), ()))
TN = (((0,), (0,)), ((), ()))


def two_parts(table):
    high = np.asarray(table, jnp.bfloat16)
    low = np.asarray(table - np.asarray(high, np.float64), jnp.bfloat16)
    return np.stack([high, low])


def signed_waves():
    index = np.arange(K)
    return np.where(index < K // 2, index, index - K)


def tables():
    angle = 2.0 * np.pi / N * (np.arange(K)[:, None] * np.arange(N)[None, :] % N)
    forward_x = np.concatenate([np.cos(angle), -np.sin(angle)], 0)
    weighting = np.where(np.arange(K) == 0, 1.0, 2.0)[:, None] / float(N) ** 3
    inverse_x = np.concatenate([np.cos(angle) * weighting, -np.sin(angle) * weighting], 0)
    one = np.arange(LOCAL)[:, None] * signed_waves()[None, :]
    both = one[:, None, :, None] + one[None, :, None, :]
    angle = 2.0 * np.pi / N * (both.reshape(CELLS, MODES) % N)
    plane = np.concatenate([np.cos(angle), -np.sin(angle)], 1)
    return two_parts(forward_x), two_parts(inverse_x), two_parts(plane)


def split(value):
    high = value.astype(jnp.bfloat16)
    low = (value - high.astype(jnp.float32)).astype(jnp.bfloat16)
    return high, low


def dot3(left, right, dims):
    dot = functools.partial(
        lax.dot_general, dimension_numbers=dims, preferred_element_type=jnp.float32
    )
    return dot(left[0], right[0]) + (dot(left[0], right[1]) + dot(left[1], right[0]))


def analyse(channel, phase, forward_x, plane, out, ready=None):
    real, imag = [], []
    for c in range(C):
        along_x = dot3(forward_x, split(channel(c)), NT)
        real.append(along_x[:K])
        imag.append(along_x[K:])
    if ready is not None:
        ready()
    both = dot3(split(jnp.concatenate(real + imag, 0)), parts(plane), NN)
    half = ROWS // 2
    part_re = both[:half, :MODES] - both[half:, MODES:]
    part_im = both[:half, MODES:] + both[half:, :MODES]
    cosine, sine = phase[0:1, :], phase[1:2, :]
    for t, part in enumerate(
        (part_re * cosine - part_im * sine, part_re * sine + part_im * cosine)
    ):
        for c in range(C):
            out[:, t * C + c, :] = part[c * K : (c + 1) * K]


def synthesise(modes_re, modes_im, phase, inverse_x, plane):
    cosine, sine = phase[0:1, :], phase[1:2, :]
    here_re = modes_re * cosine + modes_im * sine
    here_im = modes_im * cosine - modes_re * sine
    left = jnp.concatenate(
        [jnp.concatenate([here_re, here_im], 1), jnp.concatenate([here_im, -here_re], 1)], 0
    )
    lines = dot3(split(left), plane, NT)
    half = ROWS // 2
    out = []
    for c in range(C):
        pair = jnp.concatenate([lines[c * K : (c + 1) * K], lines[half + c * K :][:K]], 0)
        out.append(dot3(split(pair), inverse_x, TN))
    return out


def parts(ref):
    return ref[0], ref[1]


def analysis_kernel(fields, forward_x, plane, phase, out, cells, lines, square, arrived):
    table = pltpu.make_async_copy(forward_x, lines, arrived.at[C])
    table.start()
    copies = [
        pltpu.make_async_copy(fields.at[c], cells.at[c], arrived.at[c]) for c in range(C)
    ]
    for copy in copies:
        copy.start()
    second = pltpu.make_async_copy(plane, square, arrived.at[C + 1])
    second.start()
    table.wait()

    def channel(c):
        copies[c].wait()
        return cells[c]

    analyse(channel, phase[...], parts(lines), square, out, second.wait)


def spread_kernel(pieces, out):
    total = jnp.sum(pieces[...], axis=0)
    out[...] = jnp.broadcast_to(total[None], out.shape)


def forward_kernel(
    modes, weights, fields, cotangent, point, bias, phase, forward_x, inverse_x, plane, up, out
):
    mixed_re, mixed_im = [], []
    for o in range(C):
        re = im = 0.0
        for i in range(C):
            a, b = modes[:, i, :], modes[:, C + i, :]
            w, v = weights[0, i, o], weights[1, i, o]
            re = re + (a * w - b * v)
            im = im + (a * v + b * w)
        mixed_re.append(re)
        mixed_im.append(im)
    term = synthesise(
        jnp.concatenate(mixed_re, 0),
        jnp.concatenate(mixed_im, 0),
        phase[...],
        parts(inverse_x),
        parts(plane),
    )
    for o in range(C):
        pre = term[o] + bias[o]
        for i in range(C):
            pre = pre + point[i, o] * fields[i]
        slope = 0.5 * (1.0 + lax.erf(pre * math.sqrt(0.5))) + pre * jnp.exp(
            -0.5 * pre * pre
        ) * (1.0 / math.sqrt(2.0 * math.pi))
        up[o] = cotangent[o] * slope
    analyse(lambda c: up[c], phase[...], parts(forward_x), plane, out)


def slabs(rows, start):
    lane = lax.broadcasted_iota(jnp.int32, (8, 128), 1)
    source = (8 - lane // K) % 8 * K + lane % K
    half = jnp.take_along_axis(
        rows[:, start : start + 128], source, axis=1, mode="promise_in_bounds"
    )
    return [
        pltpu.roll(jnp.broadcast_to(half[k : k + 1], (8, 128)), 0, 1, stride=K, stride_axis=0)
        for k in range(2 * C)
    ]


def backward_kernel(
    modes,
    back,
    weights,
    up,
    point,
    phase,
    inverse_x,
    plane,
    grad_fields,
    grad_spectral,
    cells,
    stored,
    sent,
):
    copies = []

    def send(source, target):
        copies.append(pltpu.make_async_copy(source, target, sent.at[len(copies)]))
        copies[-1].start()

    def one_wave(p):
        factor = (1.0 if p == 0 else 2.0) / float(N) ** 3
        first, second = modes[p], back[p] * factor
        for half in range(2):
            u, h = slabs(first, half * 128), slabs(second, half * 128)
            for i in range(C):
                for o in range(C):
                    re = u[i] * h[o] + u[C + i] * h[C + o]
                    im = u[i] * h[C + o] - u[C + i] * h[o]
                    stored[0, i, o, p, half * 8 : half * 8 + 8, :] = re[:, :K]
                    stored[1, i, o, p, half * 8 : half * 8 + 8, :] = im[:, :K]

    for p in range(K):
        one_wave(p)
        if p % 4 == 3:
            some = pl.ds(p - 3, 4)
            send(stored.at[:, :, :, some], grad_spectral.at[:, :, :, some])
    adjoint_re, adjoint_im = [], []
    for i in range(C):
        re = im = 0.0
        for o in range(C):
            a, b = back[:, o, :], back[:, C + o, :]
            w, v = weights[0, i, o], weights[1, i, o]
            re = re + (a * w + b * v)
            im = im + (b * w - a * v)
        adjoint_re.append(re)
        adjoint_im.append(im)
    term = synthesise(
        jnp.concatenate(adjoint_re, 0),
        jnp.concatenate(adjoint_im, 0),
        phase[...],
        parts(inverse_x),
        parts(plane),
    )
    for i in range(C):
        total = term[i]
        for o in range(C):
            total = total + point[i, o] * up[o]
        cells[i] = total
        send(cells.at[i], grad_fields.at[i])
    for copy in copies:
        copy.wait()


def position_phase():
    lane = jnp.arange(MODES, dtype=jnp.int32)
    steps = (lane // K) * lax.axis_index("row") + (lane % K) * lax.axis_index("col")
    angle = (steps % K).astype(jnp.float32) * (2.0 * math.pi / K)
    return jnp.stack([jnp.cos(angle), -jnp.sin(angle)], 0)


def near(value):
    return pltpu.with_memory_space_constraint(value, pltpu.VMEM)


def far(value):
    return pltpu.with_memory_space_constraint(value, pltpu.HBM)


def near_out(shape):
    return pltpu.VMEM(shape, jnp.float32)


def groups():
    index = np.arange(256).reshape(2, 8, 4, 2, 2)
    index[1] = index[1, :, :, ::-1]
    index = index.reshape(K, K)
    return index.tolist(), index.T.tolist()


def swap(pieces, members):
    return lax.all_to_all(
        pieces, ("row", "col"), 0, 0, tiled=True, axis_index_groups=members
    )


def call(kernel, out_shape, in_specs, scratch_shapes=()):
    where = [VMEM if not isinstance(o, jax.ShapeDtypeStruct) else HBM for o in out_shape]
    return pl.pallas_call(
        kernel,
        out_shape=tuple(out_shape),
        in_specs=in_specs,
        out_specs=tuple(where),
        scratch_shapes=scratch_shapes,
        compiler_params=PARAMS,
    )


def total_modes(partial):
    shape = (K, 2 * C, MODES)
    near_by, alike = groups()
    pieces = near(swap(partial, near_by))
    (pieces,) = call(spread_kernel, [near_out(shape)], [VMEM])(pieces)
    pieces = near(swap(pieces, alike))
    (pieces,) = call(spread_kernel, [near_out(shape)], [VMEM])(pieces)
    return near(swap(pieces, near_by))


def per_device(fields, cotangent, spec_weights, point_weights, bias):
    forward_x, inverse_x, plane = [jnp.asarray(t) for t in tables()]
    shape = fields.shape
    cells = (C, CELLS, N)
    phase = near(position_phase())
    partial, fields = call(
        analysis_kernel,
        [near_out((K, 2 * C, MODES)), near_out(cells)],
        [HBM] * 3 + [VMEM],
        [
            pltpu.VMEM((2, 2 * K, N), jnp.bfloat16),
            pltpu.VMEM((2, CELLS, 2 * MODES), jnp.bfloat16),
            pltpu.SemaphoreType.DMA((C + 2,)),
        ],
    )(far(fields.reshape(cells)), far(forward_x), far(plane), phase)
    forward_x, inverse_x, plane = [near(v) for v in (forward_x, inverse_x, plane)]
    weights = near(spec_weights.reshape(2, C, C, K, MODES))
    modes = total_modes(partial)
    upstream, partial = call(
        forward_kernel,
        [near_out(cells), near_out((K, 2 * C, MODES))],
        [VMEM] * 4 + [SMEM] * 2 + [VMEM] * 4,
    )(
        modes,
        weights,
        near(fields),
        near(cotangent.reshape(cells)),
        point_weights,
        bias,
        phase,
        forward_x,
        inverse_x,
        plane,
    )
    back = total_modes(partial)
    grad_fields, grad_spectral = call(
        backward_kernel,
        [
            jax.ShapeDtypeStruct(cells, jnp.float32),
            jax.ShapeDtypeStruct((2, C, C, K, K, K), jnp.float32),
        ],
        [VMEM] * 4 + [SMEM] + [VMEM] * 3,
        [
            pltpu.VMEM(cells, jnp.float32),
            pltpu.VMEM((2, C, C, K, K, K), jnp.float32),
            pltpu.SemaphoreType.DMA((8,)),
        ],
    )(modes, back, weights, near(upstream), point_weights, phase, inverse_x, plane)
    return grad_fields.reshape(shape), grad_spectral


def solution(mesh):
    placed = P(None, None, "row", "col", None)
    return jax.shard_map(
        per_device,
        mesh=mesh,
        in_specs=(placed, placed, P(), P(), P()),
        out_specs=(placed, P()),
        check_vma=False,
    )
```

```python
import functools
import math

import jax
import jax.numpy as jnp
import numpy as np
from jax import lax
from jax.experimental import pallas as pl
from jax.experimental.pallas import tpu as pltpu
from jax.sharding import PartitionSpec as P

C = 4
N = 256
K = 16
LOCAL = 16
CELLS = LOCAL * LOCAL
MODES = K * K
ROWS = 2 * C * K

VMEM = pl.BlockSpec(memory_space=pltpu.VMEM)
HBM = pl.BlockSpec(memory_space=pltpu.HBM)
SMEM = pl.BlockSpec(memory_space=pltpu.SMEM)
PARAMS = pltpu.CompilerParams(vmem_limit_bytes=24 << 20)
NT = (((1,), (1,)), ((), ()))
NN = (((1,), (0,)), ((), ()))
TN = (((0,), (0,)), ((), ()))


def two_parts(table):
    high = np.asarray(table, jnp.bfloat16)
    low = np.asarray(table - np.asarray(high, np.float64), jnp.bfloat16)
    return np.stack([high, low])


def signed_waves():
    index = np.arange(K)
    return np.where(index < K // 2, index, index - K)


def tables():
    angle = 2.0 * np.pi / N * (np.arange(K)[:, None] * np.arange(N)[None, :] % N)
    forward_x = np.concatenate([np.cos(angle), -np.sin(angle)], 0)
    weighting = np.where(np.arange(K) == 0, 1.0, 2.0)[:, None] / float(N) ** 3
    inverse_x = np.concatenate([np.cos(angle) * weighting, -np.sin(angle) * weighting], 0)
    one = np.arange(LOCAL)[:, None] * signed_waves()[None, :]
    both = one[:, None, :, None] + one[None, :, None, :]
    angle = 2.0 * np.pi / N * (both.reshape(CELLS, MODES) % N)
    plane = np.concatenate([np.cos(angle), -np.sin(angle)], 1)
    return two_parts(forward_x), two_parts(inverse_x), two_parts(plane)


def split(value):
    high = value.astype(jnp.bfloat16)
    low = (value - high.astype(jnp.float32)).astype(jnp.bfloat16)
    return high, low


def dot3(left, right, dims):
    dot = functools.partial(
        lax.dot_general, dimension_numbers=dims, preferred_element_type=jnp.float32
    )
    return dot(left[0], right[0]) + (dot(left[0], right[1]) + dot(left[1], right[0]))


def analyse(channel, phase, forward_x, plane, out, ready=None):
    real, imag = [], []
    for c in range(C):
        along_x = dot3(forward_x, split(channel(c)), NT)
        real.append(along_x[:K])
        imag.append(along_x[K:])
    if ready is not None:
        ready()
    both = dot3(split(jnp.concatenate(real + imag, 0)), parts(plane), NN)
    half = ROWS // 2
    part_re = both[:half, :MODES] - both[half:, MODES:]
    part_im = both[:half, MODES:] + both[half:, :MODES]
    cosine, sine = phase[0:1, :], phase[1:2, :]
    for t, part in enumerate(
        (part_re * cosine - part_im * sine, part_re * sine + part_im * cosine)
    ):
        for c in range(C):
            out[:, t * C + c, :] = part[c * K : (c + 1) * K]


def synthesise(modes_re, modes_im, phase, inverse_x, plane):
    cosine, sine = phase[0:1, :], phase[1:2, :]
    here_re = modes_re * cosine + modes_im * sine
    here_im = modes_im * cosine - modes_re * sine
    left = jnp.concatenate(
        [jnp.concatenate([here_re, here_im], 1), jnp.concatenate([here_im, -here_re], 1)], 0
    )
    lines = dot3(split(left), plane, NT)
    half = ROWS // 2
    out = []
    for c in range(C):
        pair = jnp.concatenate([lines[c * K : (c + 1) * K], lines[half + c * K :][:K]], 0)
        out.append(dot3(split(pair), inverse_x, TN))
    return out


def parts(ref):
    return ref[0], ref[1]


def analysis_kernel(fields, forward_x, plane, phase, out, cells, lines, square, arrived):
    table = pltpu.make_async_copy(forward_x, lines, arrived.at[C])
    table.start()
    copies = [
        pltpu.make_async_copy(fields.at[c], cells.at[c], arrived.at[c]) for c in range(C)
    ]
    for copy in copies:
        copy.start()
    second = pltpu.make_async_copy(plane, square, arrived.at[C + 1])
    second.start()
    table.wait()

    def channel(c):
        copies[c].wait()
        return cells[c]

    analyse(channel, phase[...], parts(lines), square, out, second.wait)


def spread_kernel(pieces, out):
    total = jnp.sum(pieces[...], axis=0)
    out[...] = jnp.broadcast_to(total[None], out.shape)


def forward_kernel(
    modes, weights, fields, cotangent, point, bias, phase, forward_x, inverse_x, plane, up, out
):
    mixed_re, mixed_im = [], []
    for o in range(C):
        re = im = 0.0
        for i in range(C):
            a, b = modes[:, i, :], modes[:, C + i, :]
            w, v = weights[0, i, o], weights[1, i, o]
            re = re + (a * w - b * v)
            im = im + (a * v + b * w)
        mixed_re.append(re)
        mixed_im.append(im)
    term = synthesise(
        jnp.concatenate(mixed_re, 0),
        jnp.concatenate(mixed_im, 0),
        phase[...],
        parts(inverse_x),
        parts(plane),
    )
    for o in range(C):
        pre = term[o] + bias[o]
        for i in range(C):
            pre = pre + point[i, o] * fields[i]
        slope = 0.5 * (1.0 + lax.erf(pre * math.sqrt(0.5))) + pre * jnp.exp(
            -0.5 * pre * pre
        ) * (1.0 / math.sqrt(2.0 * math.pi))
        up[o] = cotangent[o] * slope
    analyse(lambda c: up[c], phase[...], parts(forward_x), plane, out)


def turned(modes):
    shape = (MODES, MODES)
    source, target = [lax.broadcasted_iota(jnp.int32, shape, axis) for axis in range(2)]
    wanted = target // 128 * 128 + (8 - target % 128 // K) % 8 * K + target % K
    order = (source == wanted).astype(jnp.bfloat16)
    high, rest = split_off(modes.reshape(ROWS, MODES))
    middle, rest = split_off(rest)
    total = 0.0
    for part in (rest.astype(jnp.bfloat16), middle, high):
        total = total + jnp.dot(part, order, preferred_element_type=jnp.float32)
    return total


def split_off(value):
    high = value.astype(jnp.bfloat16)
    return high, value - high.astype(jnp.float32)


def slabs(rows, start):
    half = rows[:, start : start + 128]
    return [
        pltpu.roll(jnp.broadcast_to(half[k : k + 1], (8, 128)), 0, 1, stride=K, stride_axis=0)
        for k in range(2 * C)
    ]


def backward_kernel(
    modes,
    back,
    weights,
    up,
    point,
    phase,
    inverse_x,
    plane,
    grad_fields,
    grad_spectral,
    cells,
    stored,
    sent,
):
    copies = []

    def send(source, target):
        copies.append(pltpu.make_async_copy(source, target, sent.at[len(copies)]))
        copies[-1].start()

    def one_wave(p):
        factor = (1.0 if p == 0 else 2.0) / float(N) ** 3
        first, second = [v[p * 2 * C : (p + 1) * 2 * C] for v in (modes_turned, back_turned)]
        second = second * factor
        for half in range(2):
            u, h = slabs(first, half * 128), slabs(second, half * 128)
            for i in range(C):
                for o in range(C):
                    re = u[i] * h[o] + u[C + i] * h[C + o]
                    im = u[i] * h[C + o] - u[C + i] * h[o]
                    stored[0, i, o, p, half * 8 : half * 8 + 8, :] = re[:, :K]
                    stored[1, i, o, p, half * 8 : half * 8 + 8, :] = im[:, :K]

    modes_turned, back_turned = turned(modes[...]), turned(back[...])
    for p in range(K):
        one_wave(p)
        if p % 4 == 3:
            some = pl.ds(p - 3, 4)
            send(stored.at[:, :, :, some], grad_spectral.at[:, :, :, some])
    adjoint_re, adjoint_im = [], []
    for i in range(C):
        re = im = 0.0
        for o in range(C):
            a, b = back[:, o, :], back[:, C + o, :]
            w, v = weights[0, i, o], weights[1, i, o]
            re = re + (a * w + b * v)
            im = im + (b * w - a * v)
        adjoint_re.append(re)
        adjoint_im.append(im)
    term = synthesise(
        jnp.concatenate(adjoint_re, 0),
        jnp.concatenate(adjoint_im, 0),
        phase[...],
        parts(inverse_x),
        parts(plane),
    )
    for i in range(C):
        total = term[i]
        for o in range(C):
            total = total + point[i, o] * up[o]
        cells[i] = total
        send(cells.at[i], grad_fields.at[i])
    for copy in copies:
        copy.wait()


def position_phase():
    lane = jnp.arange(MODES, dtype=jnp.int32)
    steps = (lane // K) * lax.axis_index("row") + (lane % K) * lax.axis_index("col")
    angle = (steps % K).astype(jnp.float32) * (2.0 * math.pi / K)
    return jnp.stack([jnp.cos(angle), -jnp.sin(angle)], 0)


def near(value):
    return pltpu.with_memory_space_constraint(value, pltpu.VMEM)


def far(value):
    return pltpu.with_memory_space_constraint(value, pltpu.HBM)


def near_out(shape):
    return pltpu.VMEM(shape, jnp.float32)


def groups():
    index = np.arange(256).reshape(2, 8, 4, 2, 2)
    index[1] = index[1, :, :, ::-1]
    index = index.reshape(K, K)
    return index.tolist(), index.T.tolist()


def swap(pieces, members):
    return lax.all_to_all(
        pieces, ("row", "col"), 0, 0, tiled=True, axis_index_groups=members
    )


def call(kernel, out_shape, in_specs, scratch_shapes=()):
    where = [VMEM if not isinstance(o, jax.ShapeDtypeStruct) else HBM for o in out_shape]
    return pl.pallas_call(
        kernel,
        out_shape=tuple(out_shape),
        in_specs=in_specs,
        out_specs=tuple(where),
        scratch_shapes=scratch_shapes,
        compiler_params=PARAMS,
    )


def total_modes(partial):
    shape = (K, 2 * C, MODES)
    near_by, alike = groups()
    pieces = near(swap(partial, near_by))
    (pieces,) = call(spread_kernel, [near_out(shape)], [VMEM])(pieces)
    pieces = near(swap(pieces, alike))
    (pieces,) = call(spread_kernel, [near_out(shape)], [VMEM])(pieces)
    return near(swap(pieces, near_by))


def per_device(fields, cotangent, spec_weights, point_weights, bias):
    forward_x, inverse_x, plane = [jnp.asarray(t) for t in tables()]
    shape = fields.shape
    cells = (C, CELLS, N)
    phase = near(position_phase())
    partial, fields = call(
        analysis_kernel,
        [near_out((K, 2 * C, MODES)), near_out(cells)],
        [HBM] * 3 + [VMEM],
        [
            pltpu.VMEM((2, 2 * K, N), jnp.bfloat16),
            pltpu.VMEM((2, CELLS, 2 * MODES), jnp.bfloat16),
            pltpu.SemaphoreType.DMA((C + 2,)),
        ],
    )(far(fields.reshape(cells)), far(forward_x), far(plane), phase)
    forward_x, inverse_x, plane = [near(v) for v in (forward_x, inverse_x, plane)]
    weights = near(spec_weights.reshape(2, C, C, K, MODES))
    modes = total_modes(partial)
    upstream, partial = call(
        forward_kernel,
        [near_out(cells), near_out((K, 2 * C, MODES))],
        [VMEM] * 4 + [SMEM] * 2 + [VMEM] * 4,
    )(
        modes,
        weights,
        near(fields),
        near(cotangent.reshape(cells)),
        point_weights,
        bias,
        phase,
        forward_x,
        inverse_x,
        plane,
    )
    back = total_modes(partial)
    grad_fields, grad_spectral = call(
        backward_kernel,
        [
            jax.ShapeDtypeStruct(cells, jnp.float32),
            jax.ShapeDtypeStruct((2, C, C, K, K, K), jnp.float32),
        ],
        [VMEM] * 4 + [SMEM] + [VMEM] * 3,
        [
            pltpu.VMEM(cells, jnp.float32),
            pltpu.VMEM((2, C, C, K, K, K), jnp.float32),
            pltpu.SemaphoreType.DMA((8,)),
        ],
    )(modes, back, weights, near(upstream), point_weights, phase, inverse_x, plane)
    return grad_fields.reshape(shape), grad_spectral


def solution(mesh):
    placed = P(None, None, "row", "col", None)
    return jax.shard_map(
        per_device,
        mesh=mesh,
        in_specs=(placed, placed, P(), P(), P()),
        out_specs=(placed, P()),
        check_vma=False,
    )
```

```python
import functools
import math

import jax
import jax.numpy as jnp
import numpy as np
from jax import lax
from jax.experimental import pallas as pl
from jax.experimental.pallas import tpu as pltpu
from jax.sharding import PartitionSpec as P

C = 4
N = 256
K = 16
LOCAL = 16
CELLS = LOCAL * LOCAL
MODES = K * K
ROWS = 2 * C * K
HALF_ROOT = math.sqrt(0.5)

VMEM = pl.BlockSpec(memory_space=pltpu.VMEM)
HBM = pl.BlockSpec(memory_space=pltpu.HBM)
SMEM = pl.BlockSpec(memory_space=pltpu.SMEM)
PARAMS = pltpu.CompilerParams(vmem_limit_bytes=24 << 20)
NT = (((1,), (1,)), ((), ()))
NN = (((1,), (0,)), ((), ()))
TN = (((0,), (0,)), ((), ()))


def two_parts(table):
    high = np.asarray(table, jnp.bfloat16)
    low = np.asarray(table - np.asarray(high, np.float64), jnp.bfloat16)
    return np.stack([high, low])


def joined(table):
    high, low = two_parts(table)
    return np.concatenate([high, high, low], 0)


def signed_waves():
    index = np.arange(K)
    return np.where(index < K // 2, index, index - K)


def tables():
    angle = 2.0 * np.pi / N * (np.arange(K)[:, None] * np.arange(N)[None, :] % N)
    forward_x = np.concatenate([np.cos(angle), -np.sin(angle)], 0)
    weighting = np.where(np.arange(K) == 0, 1.0, 2.0)[:, None] / float(N) ** 3
    inverse_x = np.concatenate([np.cos(angle) * weighting, -np.sin(angle) * weighting], 0)
    one = np.arange(LOCAL)[:, None] * signed_waves()[None, :]
    both = one[:, None, :, None] + one[None, :, None, :]
    angle = 2.0 * np.pi / N * (both.reshape(CELLS, MODES) % N)
    plane = np.concatenate([np.cos(angle), -np.sin(angle)], 1)
    scaled_x, inverse_x = joined(inverse_x * np.sqrt(0.5)), joined(inverse_x * 0.5)
    return two_parts(forward_x), scaled_x, inverse_x, two_parts(plane)


def split(value):
    high = value.astype(jnp.bfloat16)
    low = (value - high.astype(jnp.float32)).astype(jnp.bfloat16)
    return high, low


def dot_of(dims):
    return functools.partial(
        lax.dot_general, dimension_numbers=dims, preferred_element_type=jnp.float32
    )


def dot3(left, right, dims):
    dot = dot_of(dims)
    rows = left[0].shape[0]
    both = dot(jnp.concatenate(left, 0), right[0])
    return both[:rows] + (dot(left[0], right[1]) + both[rows:])


def analyse(channel, phase, forward_x, plane, out, ready=None):
    real, imag = [], []
    for c in range(C):
        along_x = dot3(forward_x, split(channel(c)), NT)
        real.append(along_x[:K])
        imag.append(along_x[K:])
    if ready is not None:
        ready()
    both = dot3(split(jnp.concatenate(real + imag, 0)), parts(plane), NN)
    half = ROWS // 2
    part_re = both[:half, :MODES] - both[half:, MODES:]
    part_im = both[:half, MODES:] + both[half:, :MODES]
    cosine, sine = phase[0:1, :], phase[1:2, :]
    for t, part in enumerate(
        (part_re * cosine - part_im * sine, part_re * sine + part_im * cosine)
    ):
        for c in range(C):
            out[:, t * C + c, :] = part[c * K : (c + 1) * K]


def synthesise(modes_re, modes_im, phase, inverse_x, plane):
    cosine, sine = phase[0:1, :], phase[1:2, :]
    here_re = modes_re * cosine + modes_im * sine
    here_im = modes_im * cosine - modes_re * sine
    left = jnp.concatenate(
        [jnp.concatenate([here_re, here_im], 1), jnp.concatenate([here_im, -here_re], 1)], 0
    )
    lines = dot3(split(left), plane, NT)
    half = ROWS // 2
    out = []
    for c in range(C):
        pair = jnp.concatenate([lines[c * K : (c + 1) * K], lines[half + c * K :][:K]], 0)
        high, low = split(pair)
        out.append(dot_of(TN)(jnp.concatenate([high, low, high], 0), inverse_x))
    return out


def parts(ref):
    return ref[0], ref[1]


def analysis_kernel(fields, forward_x, plane, phase, out, lines, square, cells, arrived):
    table = pltpu.make_async_copy(forward_x, lines, arrived.at[C])
    table.start()
    copies = [
        pltpu.make_async_copy(fields.at[c], cells.at[c], arrived.at[c]) for c in range(C)
    ]
    for copy in copies:
        copy.start()
    second = pltpu.make_async_copy(plane, square, arrived.at[C + 1])
    second.start()
    table.wait()

    def channel(c):
        copies[c].wait()
        return cells[c]

    analyse(channel, phase[...], parts(lines), square, out, second.wait)


def spread_kernel(pieces, out):
    total = jnp.sum(pieces[...], axis=0)
    out[...] = jnp.broadcast_to(total[None], out.shape)


def local_kernel(fields, upper, point, bias, out, cotangent, cells, arrived):
    copies = [
        pltpu.make_async_copy(fields.at[c], cells.at[c], arrived.at[c]) for c in range(C)
    ]
    copies.append(pltpu.make_async_copy(upper, cotangent, arrived.at[C]))
    for copy in copies:
        copy.start()
    for copy in copies[:C]:
        copy.wait()
    for o in range(C):
        total = bias[o] * HALF_ROOT
        for i in range(C):
            total = total + (point[i, o] * HALF_ROOT) * cells[i]
        out[o] = total
    copies[C].wait()


def forward_kernel(
    modes, weights, local, cotangent, phase, forward_x, scaled_x, plane, up, out
):
    mixed_re, mixed_im = [], []
    for o in range(C):
        re = im = 0.0
        for i in range(C):
            a, b = modes[:, i, :], modes[:, C + i, :]
            w, v = weights[0, i, o], weights[1, i, o]
            re = re + (a * w - b * v)
            im = im + (a * v + b * w)
        mixed_re.append(re)
        mixed_im.append(im)
    term = synthesise(
        jnp.concatenate(mixed_re, 0),
        jnp.concatenate(mixed_im, 0),
        phase[...],
        scaled_x[...],
        parts(plane),
    )
    for o in range(C):
        s = term[o] + local[o]
        bell = jnp.exp2(s * s * (-1.0 / math.log(2.0)))
        up[o] = cotangent[o] * ((1.0 + lax.erf(s)) + s * (2.0 / math.sqrt(math.pi)) * bell)
    analyse(lambda c: up[c], phase[...], parts(forward_x), plane, out)


def turned(modes):
    shape = (MODES, MODES)
    source, target = [lax.broadcasted_iota(jnp.int32, shape, axis) for axis in range(2)]
    wanted = target // 128 * 128 + (8 - target % 128 // K) % 8 * K + target % K
    order = (source == wanted).astype(jnp.bfloat16)
    high, rest = split_off(modes.reshape(ROWS, MODES))
    middle, rest = split_off(rest)
    total = 0.0
    for part in (rest.astype(jnp.bfloat16), middle, high):
        total = total + jnp.dot(part, order, preferred_element_type=jnp.float32)
    return total


def split_off(value):
    high = value.astype(jnp.bfloat16)
    return high, value - high.astype(jnp.float32)


def slabs(rows, start):
    half = rows[:, start : start + 128]
    return [
        pltpu.roll(jnp.broadcast_to(half[k : k + 1], (8, 128)), 0, 1, stride=K, stride_axis=0)
        for k in range(2 * C)
    ]


def backward_kernel(
    modes,
    back,
    weights,
    up,
    point,
    phase,
    inverse_x,
    plane,
    grad_fields,
    grad_spectral,
    cells,
    stored,
    sent,
):
    copies = []

    def send(source, target):
        copies.append(pltpu.make_async_copy(source, target, sent.at[len(copies)]))
        copies[-1].start()

    def one_wave(p):
        factor = (0.5 if p == 0 else 1.0) / float(N) ** 3
        first, second = [v[p * 2 * C : (p + 1) * 2 * C] for v in (modes_turned, back_turned)]
        second = second * factor
        for half in range(2):
            u, h = slabs(first, half * 128), slabs(second, half * 128)
            for i in range(C):
                for o in range(C):
                    re = u[i] * h[o] + u[C + i] * h[C + o]
                    im = u[i] * h[C + o] - u[C + i] * h[o]
                    stored[0, i, o, p, half * 8 : half * 8 + 8, :] = re[:, :K]
                    stored[1, i, o, p, half * 8 : half * 8 + 8, :] = im[:, :K]

    modes_turned, back_turned = turned(modes[...]), turned(back[...])
    for p in range(K):
        one_wave(p)
        if p % 4 == 3:
            some = pl.ds(p - 3, 4)
            send(stored.at[:, :, :, some], grad_spectral.at[:, :, :, some])
    adjoint_re, adjoint_im = [], []
    for i in range(C):
        re = im = 0.0
        for o in range(C):
            a, b = back[:, o, :], back[:, C + o, :]
            w, v = weights[0, i, o], weights[1, i, o]
            re = re + (a * w + b * v)
            im = im + (b * w - a * v)
        adjoint_re.append(re)
        adjoint_im.append(im)
    term = synthesise(
        jnp.concatenate(adjoint_re, 0),
        jnp.concatenate(adjoint_im, 0),
        phase[...],
        inverse_x[...],
        parts(plane),
    )
    for i in range(C):
        total = term[i]
        for o in range(C):
            total = total + (point[i, o] * 0.5) * up[o]
        cells[i] = total
        send(cells.at[i], grad_fields.at[i])
    for copy in copies:
        copy.wait()


def position_phase():
    lane = jnp.arange(MODES, dtype=jnp.int32)
    steps = (lane // K) * lax.axis_index("row") + (lane % K) * lax.axis_index("col")
    angle = (steps % K).astype(jnp.float32) * (2.0 * math.pi / K)
    return jnp.stack([jnp.cos(angle), -jnp.sin(angle)], 0)


def near(value):
    return pltpu.with_memory_space_constraint(value, pltpu.VMEM)


def far(value):
    return pltpu.with_memory_space_constraint(value, pltpu.HBM)


def near_out(shape, dtype=jnp.float32):
    return pltpu.VMEM(shape, dtype)


def groups():
    index = np.arange(256).reshape(2, 8, 4, 2, 2)
    index[1] = index[1, :, :, ::-1]
    index = index.reshape(K, K)
    return index.tolist(), index.T.tolist()


def swap(pieces, members):
    return lax.all_to_all(
        pieces, ("row", "col"), 0, 0, tiled=True, axis_index_groups=members
    )


def call(kernel, out_shape, in_specs, scratch_shapes=()):
    where = [VMEM if not isinstance(o, jax.ShapeDtypeStruct) else HBM for o in out_shape]
    return pl.pallas_call(
        kernel,
        out_shape=tuple(out_shape),
        in_specs=in_specs,
        out_specs=tuple(where),
        scratch_shapes=scratch_shapes,
        compiler_params=PARAMS,
    )


def total_modes(partial):
    shape = (K, 2 * C, MODES)
    near_by, alike = groups()
    pieces = near(swap(partial, near_by))
    (pieces,) = call(spread_kernel, [near_out(shape)], [VMEM])(pieces)
    pieces = near(swap(pieces, alike))
    (pieces,) = call(spread_kernel, [near_out(shape)], [VMEM])(pieces)
    return near(swap(pieces, near_by))


def per_device(fields, cotangent, spec_weights, point_weights, bias):
    forward_x, scaled_x, inverse_x, plane = [jnp.asarray(t) for t in tables()]
    shape = fields.shape
    cells = (C, CELLS, N)
    phase = near(position_phase())
    partial, forward_x, plane = call(
        analysis_kernel,
        [
            near_out((K, 2 * C, MODES)),
            near_out(forward_x.shape, jnp.bfloat16),
            near_out(plane.shape, jnp.bfloat16),
        ],
        [HBM] * 3 + [VMEM],
        [pltpu.VMEM(cells, jnp.float32), pltpu.SemaphoreType.DMA((C + 2,))],
    )(far(fields.reshape(cells)), far(forward_x), far(plane), phase)
    forward_x, scaled_x, inverse_x, plane = [
        near(v) for v in (forward_x, scaled_x, inverse_x, plane)
    ]
    weights = near(spec_weights.reshape(2, C, C, K, MODES))
    modes = total_modes(partial)
    local, cotangent = call(
        local_kernel,
        [near_out(cells)] * 2,
        [HBM] * 2 + [SMEM] * 2,
        [pltpu.VMEM(cells, jnp.float32), pltpu.SemaphoreType.DMA((C + 1,))],
    )(far(fields.reshape(cells)), far(cotangent.reshape(cells)), point_weights, bias)
    upstream, partial = call(
        forward_kernel,
        [near_out(cells), near_out((K, 2 * C, MODES))],
        [VMEM] * 8,
    )(modes, weights, near(local), near(cotangent), phase, forward_x, scaled_x, plane)
    back = total_modes(partial)
    grad_fields, grad_spectral = call(
        backward_kernel,
        [
            jax.ShapeDtypeStruct(cells, jnp.float32),
            jax.ShapeDtypeStruct((2, C, C, K, K, K), jnp.float32),
        ],
        [VMEM] * 4 + [SMEM] + [VMEM] * 3,
        [
            pltpu.VMEM(cells, jnp.float32),
            pltpu.VMEM((2, C, C, K, K, K), jnp.float32),
            pltpu.SemaphoreType.DMA((8,)),
        ],
    )(modes, back, weights, near(upstream), point_weights, phase, inverse_x, plane)
    return grad_fields.reshape(shape), grad_spectral


def solution(mesh):
    placed = P(None, None, "row", "col", None)
    return jax.shard_map(
        per_device,
        mesh=mesh,
        in_specs=(placed, placed, P(), P(), P()),
        out_specs=(placed, P()),
        check_vma=False,
    )
```

```python
import functools
import math

import jax
import jax.numpy as jnp
import numpy as np
from jax import lax
from jax.experimental import pallas as pl
from jax.experimental.pallas import tpu as pltpu
from jax.sharding import PartitionSpec as P

C = 4
N = 256
K = 16
LOCAL = 16
CELLS = LOCAL * LOCAL
MODES = K * K
ROWS = 2 * C * K
HALF_ROOT = math.sqrt(0.5)

VMEM = pl.BlockSpec(memory_space=pltpu.VMEM)
HBM = pl.BlockSpec(memory_space=pltpu.HBM)
SMEM = pl.BlockSpec(memory_space=pltpu.SMEM)
PARAMS = pltpu.CompilerParams(vmem_limit_bytes=24 << 20)
NT = (((1,), (1,)), ((), ()))
NN = (((1,), (0,)), ((), ()))
TN = (((0,), (0,)), ((), ()))


def two_parts(table):
    high = np.asarray(table, jnp.bfloat16)
    low = np.asarray(table - np.asarray(high, np.float64), jnp.bfloat16)
    return np.stack([high, low])


def joined(table):
    high, low = two_parts(table)
    return np.concatenate([high, high, low], 0)


def signed_waves():
    index = np.arange(K)
    return np.where(index < K // 2, index, index - K)


def tables():
    angle = 2.0 * np.pi / N * (np.arange(K)[:, None] * np.arange(N)[None, :] % N)
    forward_x = np.concatenate([np.cos(angle), -np.sin(angle)], 0)
    weighting = np.where(np.arange(K) == 0, 1.0, 2.0)[:, None] / float(N) ** 3
    inverse_x = np.concatenate([np.cos(angle) * weighting, -np.sin(angle) * weighting], 0)
    one = np.arange(LOCAL)[:, None] * signed_waves()[None, :]
    both = one[:, None, :, None] + one[None, :, None, :]
    angle = 2.0 * np.pi / N * (both.reshape(CELLS, MODES) % N)
    plane = np.concatenate([np.cos(angle), -np.sin(angle)], 1)
    scaled_x, inverse_x = joined(inverse_x * np.sqrt(0.5)), joined(inverse_x * 0.5)
    return two_parts(forward_x), scaled_x, inverse_x, two_parts(plane)


def split(value):
    high = value.astype(jnp.bfloat16)
    low = (value - high.astype(jnp.float32)).astype(jnp.bfloat16)
    return high, low


def dot_of(dims):
    return functools.partial(
        lax.dot_general, dimension_numbers=dims, preferred_element_type=jnp.float32
    )


def dot3(left, right, dims):
    dot = dot_of(dims)
    rows = left[0].shape[0]
    both = dot(jnp.concatenate(left, 0), right[0])
    return both[:rows] + (dot(left[0], right[1]) + both[rows:])


def analyse(channel, phase, forward_x, plane, out, ready=None):
    real, imag = [], []
    for c in range(C):
        along_x = dot3(forward_x, split(channel(c)), NT)
        real.append(along_x[:K])
        imag.append(along_x[K:])
    if ready is not None:
        ready()
    both = dot3(split(jnp.concatenate(real + imag, 0)), parts(plane), NN)
    half = ROWS // 2
    part_re = both[:half, :MODES] - both[half:, MODES:]
    part_im = both[:half, MODES:] + both[half:, :MODES]
    cosine, sine = phase[0:1, :], phase[1:2, :]
    for t, part in enumerate(
        (part_re * cosine - part_im * sine, part_re * sine + part_im * cosine)
    ):
        for c in range(C):
            out[:, t * C + c, :] = part[c * K : (c + 1) * K]


def synthesise(modes_re, modes_im, phase, inverse_x, plane):
    cosine, sine = phase[0:1, :], phase[1:2, :]
    here_re = modes_re * cosine + modes_im * sine
    here_im = modes_im * cosine - modes_re * sine
    left = jnp.concatenate(
        [jnp.concatenate([here_re, here_im], 1), jnp.concatenate([here_im, -here_re], 1)], 0
    )
    lines = dot3(split(left), plane, NT)
    half = ROWS // 2
    out = []
    for c in range(C):
        pair = jnp.concatenate([lines[c * K : (c + 1) * K], lines[half + c * K :][:K]], 0)
        high, low = split(pair)
        out.append(dot_of(TN)(jnp.concatenate([high, low, high], 0), inverse_x))
    return out


def parts(ref):
    return ref[0], ref[1]


def analysis_kernel(fields, forward_x, plane, phase, out, cells, lines, square, arrived):
    table = pltpu.make_async_copy(forward_x, lines, arrived.at[C])
    table.start()
    copies = [
        pltpu.make_async_copy(fields.at[c], cells.at[c], arrived.at[c]) for c in range(C)
    ]
    for copy in copies:
        copy.start()
    second = pltpu.make_async_copy(plane, square, arrived.at[C + 1])
    second.start()
    table.wait()

    def channel(c):
        copies[c].wait()
        return cells[c]

    analyse(channel, phase[...], parts(lines), square, out, second.wait)


def spread_kernel(pieces, out):
    total = jnp.sum(pieces[...], axis=0)
    out[...] = jnp.broadcast_to(total[None], out.shape)


def local_kernel(fields, point, bias, out):
    del fields
    for start in range(0, CELLS, 8):
        cells = [out[i, start : start + 8] for i in range(C)]
        for o in range(C):
            total = bias[o] * HALF_ROOT
            for i in range(C):
                total = total + (point[i, o] * HALF_ROOT) * cells[i]
            out[o, start : start + 8] = total


def forward_kernel(
    modes, weights, local, cotangent, phase, forward_x, scaled_x, plane, up, out
):
    mixed_re, mixed_im = [], []
    for o in range(C):
        re = im = 0.0
        for i in range(C):
            a, b = modes[:, i, :], modes[:, C + i, :]
            w, v = weights[0, i, o], weights[1, i, o]
            re = re + (a * w - b * v)
            im = im + (a * v + b * w)
        mixed_re.append(re)
        mixed_im.append(im)
    term = synthesise(
        jnp.concatenate(mixed_re, 0),
        jnp.concatenate(mixed_im, 0),
        phase[...],
        scaled_x[...],
        parts(plane),
    )
    for o in range(C):
        s = term[o] + local[o]
        bell = jnp.exp2(s * s * (-1.0 / math.log(2.0)))
        up[o] = cotangent[o] * ((1.0 + lax.erf(s)) + s * (2.0 / math.sqrt(math.pi)) * bell)
    analyse(lambda c: up[c], phase[...], parts(forward_x), plane, out)


def turned(modes):
    shape = (MODES, MODES)
    source, target = [lax.broadcasted_iota(jnp.int32, shape, axis) for axis in range(2)]
    wanted = target // 128 * 128 + (8 - target % 128 // K) % 8 * K + target % K
    order = (source == wanted).astype(jnp.bfloat16)
    high, rest = split_off(modes.reshape(ROWS, MODES))
    middle, rest = split_off(rest)
    total = 0.0
    for part in (rest.astype(jnp.bfloat16), middle, high):
        total = total + jnp.dot(part, order, preferred_element_type=jnp.float32)
    return total


def split_off(value):
    high = value.astype(jnp.bfloat16)
    return high, value - high.astype(jnp.float32)


def slabs(rows, start):
    half = rows[:, start : start + 128]
    return [
        pltpu.roll(jnp.broadcast_to(half[k : k + 1], (8, 128)), 0, 1, stride=K, stride_axis=0)
        for k in range(2 * C)
    ]


def backward_kernel(
    modes,
    back,
    weights,
    up,
    point,
    phase,
    inverse_x,
    plane,
    grad_fields,
    grad_spectral,
    cells,
    stored,
    sent,
):
    copies = []

    def send(source, target):
        copies.append(pltpu.make_async_copy(source, target, sent.at[len(copies)]))
        copies[-1].start()

    def one_wave(p):
        factor = (0.5 if p == 0 else 1.0) / float(N) ** 3
        first, second = [v[p * 2 * C : (p + 1) * 2 * C] for v in (modes_turned, back_turned)]
        second = second * factor
        for half in range(2):
            u, h = slabs(first, half * 128), slabs(second, half * 128)
            for i in range(C):
                for o in range(C):
                    re = u[i] * h[o] + u[C + i] * h[C + o]
                    im = u[i] * h[C + o] - u[C + i] * h[o]
                    stored[0, i, o, p, half * 8 : half * 8 + 8, :] = re[:, :K]
                    stored[1, i, o, p, half * 8 : half * 8 + 8, :] = im[:, :K]

    modes_turned, back_turned = turned(modes[...]), turned(back[...])
    for p in range(K):
        one_wave(p)
        if p % 4 == 3:
            some = pl.ds(p - 3, 4)
            send(stored.at[:, :, :, some], grad_spectral.at[:, :, :, some])
    adjoint_re, adjoint_im = [], []
    for i in range(C):
        re = im = 0.0
        for o in range(C):
            a, b = back[:, o, :], back[:, C + o, :]
            w, v = weights[0, i, o], weights[1, i, o]
            re = re + (a * w + b * v)
            im = im + (b * w - a * v)
        adjoint_re.append(re)
        adjoint_im.append(im)
    term = synthesise(
        jnp.concatenate(adjoint_re, 0),
        jnp.concatenate(adjoint_im, 0),
        phase[...],
        inverse_x[...],
        parts(plane),
    )
    for i in range(C):
        total = term[i]
        for o in range(C):
            total = total + (point[i, o] * 0.5) * up[o]
        cells[i] = total
        send(cells.at[i], grad_fields.at[i])
    for copy in copies:
        copy.wait()


def position_phase():
    lane = jnp.arange(MODES, dtype=jnp.int32)
    steps = (lane // K) * lax.axis_index("row") + (lane % K) * lax.axis_index("col")
    angle = (steps % K).astype(jnp.float32) * (2.0 * math.pi / K)
    return jnp.stack([jnp.cos(angle), -jnp.sin(angle)], 0)


def near(value):
    return pltpu.with_memory_space_constraint(value, pltpu.VMEM)


def far(value):
    return pltpu.with_memory_space_constraint(value, pltpu.HBM)


def near_out(shape, dtype=jnp.float32):
    return pltpu.VMEM(shape, dtype)


def groups():
    index = np.arange(256).reshape(2, 8, 4, 2, 2)
    index[1] = index[1, :, :, ::-1]
    index = index.reshape(K, K)
    return index.tolist(), index.T.tolist()


def swap(pieces, members):
    return lax.all_to_all(
        pieces, ("row", "col"), 0, 0, tiled=True, axis_index_groups=members
    )


def call(kernel, out_shape, in_specs, scratch_shapes=(), **more):
    where = [VMEM if not isinstance(o, jax.ShapeDtypeStruct) else HBM for o in out_shape]
    return pl.pallas_call(
        kernel,
        out_shape=tuple(out_shape),
        in_specs=in_specs,
        out_specs=tuple(where),
        scratch_shapes=scratch_shapes,
        compiler_params=PARAMS,
        **more,
    )


def total_modes(partial):
    shape = (K, 2 * C, MODES)
    near_by, alike = groups()
    pieces = near(swap(partial, near_by))
    (pieces,) = call(spread_kernel, [near_out(shape)], [VMEM])(pieces)
    pieces = near(swap(pieces, alike))
    (pieces,) = call(spread_kernel, [near_out(shape)], [VMEM])(pieces)
    return near(swap(pieces, near_by))


def per_device(fields, cotangent, spec_weights, point_weights, bias):
    forward_x, scaled_x, inverse_x, plane = [jnp.asarray(t) for t in tables()]
    shape = fields.shape
    cells = (C, CELLS, N)
    phase = near(position_phase())
    partial, fields, forward_x, plane = call(
        analysis_kernel,
        [
            near_out((K, 2 * C, MODES)),
            near_out(cells),
            near_out(forward_x.shape, jnp.bfloat16),
            near_out(plane.shape, jnp.bfloat16),
        ],
        [HBM] * 3 + [VMEM],
        [pltpu.SemaphoreType.DMA((C + 2,))],
    )(far(fields.reshape(cells)), far(forward_x), far(plane), phase)
    partial, cotangent = lax.optimization_barrier((partial, cotangent))
    fields, cotangent, forward_x, scaled_x, inverse_x, plane = [
        near(v)
        for v in (fields, cotangent.reshape(cells), forward_x, scaled_x, inverse_x, plane)
    ]
    weights = near(spec_weights.reshape(2, C, C, K, MODES))
    modes = total_modes(partial)
    (local,) = call(
        local_kernel, [near_out(cells)], [VMEM] + [SMEM] * 2, input_output_aliases={0: 0}
    )(fields, point_weights, bias)
    upstream, partial = call(
        forward_kernel,
        [near_out(cells), near_out((K, 2 * C, MODES))],
        [VMEM] * 8,
    )(modes, weights, near(local), cotangent, phase, forward_x, scaled_x, plane)
    back = total_modes(partial)
    grad_fields, grad_spectral = call(
        backward_kernel,
        [
            jax.ShapeDtypeStruct(cells, jnp.float32),
            jax.ShapeDtypeStruct((2, C, C, K, K, K), jnp.float32),
        ],
        [VMEM] * 4 + [SMEM] + [VMEM] * 3,
        [
            pltpu.VMEM(cells, jnp.float32),
            pltpu.VMEM((2, C, C, K, K, K), jnp.float32),
            pltpu.SemaphoreType.DMA((8,)),
        ],
    )(modes, back, weights, near(upstream), point_weights, phase, inverse_x, plane)
    return grad_fields.reshape(shape), grad_spectral


def solution(mesh):
    placed = P(None, None, "row", "col", None)
    return jax.shard_map(
        per_device,
        mesh=mesh,
        in_specs=(placed, placed, P(), P(), P()),
        out_specs=(placed, P()),
        check_vma=False,
    )
```

```python
import functools
import math

import jax
import jax.numpy as jnp
import numpy as np
from jax import lax
from jax.experimental import pallas as pl
from jax.experimental.pallas import tpu as pltpu
from jax.sharding import PartitionSpec as P

C = 4
N = 256
K = 16
LOCAL = 16
CELLS = LOCAL * LOCAL
MODES = K * K
ROWS = 2 * C * K
HALF_ROOT = math.sqrt(0.5)

VMEM = pl.BlockSpec(memory_space=pltpu.VMEM)
HBM = pl.BlockSpec(memory_space=pltpu.HBM)
SMEM = pl.BlockSpec(memory_space=pltpu.SMEM)
PARAMS = pltpu.CompilerParams(vmem_limit_bytes=24 << 20)
NT = (((1,), (1,)), ((), ()))
NN = (((1,), (0,)), ((), ()))
TN = (((0,), (0,)), ((), ()))


def two_parts(table):
    high = np.asarray(table, jnp.bfloat16)
    low = np.asarray(table - np.asarray(high, np.float64), jnp.bfloat16)
    return np.stack([high, low])


def joined(table):
    high, low = two_parts(table)
    return np.concatenate([high, high, low], 0)


def signed_waves():
    index = np.arange(K)
    return np.where(index < K // 2, index, index - K)


def tables():
    angle = 2.0 * np.pi / N * (np.arange(K)[:, None] * np.arange(N)[None, :] % N)
    forward_x = np.concatenate([np.cos(angle), -np.sin(angle)], 0)
    weighting = np.where(np.arange(K) == 0, 1.0, 2.0)[:, None] / float(N) ** 3
    inverse_x = np.concatenate([np.cos(angle) * weighting, -np.sin(angle) * weighting], 0)
    one = np.arange(LOCAL)[:, None] * signed_waves()[None, :]
    both = one[:, None, :, None] + one[None, :, None, :]
    angle = 2.0 * np.pi / N * (both.reshape(CELLS, MODES) % N)
    plane = np.concatenate([np.cos(angle), -np.sin(angle)], 1)
    scaled_x, inverse_x = joined(inverse_x * np.sqrt(0.5)), joined(inverse_x * 0.5)
    return two_parts(forward_x), scaled_x, inverse_x, two_parts(plane)


def split(value):
    high = value.astype(jnp.bfloat16)
    low = (value - high.astype(jnp.float32)).astype(jnp.bfloat16)
    return high, low


def dot_of(dims):
    return functools.partial(
        lax.dot_general, dimension_numbers=dims, preferred_element_type=jnp.float32
    )


def dot3(left, right, dims):
    dot = dot_of(dims)
    rows = left[0].shape[0]
    both = dot(jnp.concatenate(left, 0), right[0])
    return both[:rows] + (dot(left[0], right[1]) + both[rows:])


def analyse(channel, phase, forward_x, plane, out, ready=None):
    real, imag = [], []
    for c in range(C):
        along_x = dot3(forward_x, split(channel(c)), NT)
        real.append(along_x[:K])
        imag.append(along_x[K:])
    if ready is not None:
        ready()
    both = dot3(split(jnp.concatenate(real + imag, 0)), parts(plane), NN)
    half = ROWS // 2
    part_re = both[:half, :MODES] - both[half:, MODES:]
    part_im = both[:half, MODES:] + both[half:, :MODES]
    cosine, sine = phase[0:1, :], phase[1:2, :]
    for t, part in enumerate(
        (part_re * cosine - part_im * sine, part_re * sine + part_im * cosine)
    ):
        for c in range(C):
            out[:, t * C + c, :] = part[c * K : (c + 1) * K]


def synthesise(modes_re, modes_im, phase, inverse_x, plane):
    cosine, sine = phase[0:1, :], phase[1:2, :]
    here_re = modes_re * cosine + modes_im * sine
    here_im = modes_im * cosine - modes_re * sine
    left = jnp.concatenate(
        [jnp.concatenate([here_re, here_im], 1), jnp.concatenate([here_im, -here_re], 1)], 0
    )
    lines = dot3(split(left), plane, NT)
    half = ROWS // 2
    out = []
    for c in range(C):
        pair = jnp.concatenate([lines[c * K : (c + 1) * K], lines[half + c * K :][:K]], 0)
        high, low = split(pair)
        out.append(dot_of(TN)(jnp.concatenate([high, low, high], 0), inverse_x))
    return out


def parts(ref):
    return ref[0], ref[1]


def analysis_kernel(fields, forward_x, plane, phase, out, cells, lines, square, arrived):
    table = pltpu.make_async_copy(forward_x, lines, arrived.at[C])
    table.start()
    copies = [
        pltpu.make_async_copy(fields.at[c], cells.at[c], arrived.at[c]) for c in range(C)
    ]
    for copy in copies:
        copy.start()
    second = pltpu.make_async_copy(plane, square, arrived.at[C + 1])
    second.start()
    table.wait()

    def channel(c):
        copies[c].wait()
        return cells[c]

    analyse(channel, phase[...], parts(lines), square, out, second.wait)


def spread_kernel(pieces, out):
    total = jnp.sum(pieces[...], axis=0)
    out[...] = jnp.broadcast_to(total[None], out.shape)


def local_kernel(fields, point, bias, out):
    del fields
    for start in range(0, CELLS, 8):
        cells = [out[i, start : start + 8] for i in range(C)]
        for o in range(C):
            total = bias[o] * HALF_ROOT
            for i in range(C):
                total = total + (point[i, o] * HALF_ROOT) * cells[i]
            out[o, start : start + 8] = total


def forward_kernel(
    modes, weights, local, cotangent, phase, forward_x, scaled_x, plane, up, out
):
    mixed_re, mixed_im = [], []
    for o in range(C):
        re = im = 0.0
        for i in range(C):
            a, b = modes[:, i, :], modes[:, C + i, :]
            w, v = weights[0, i, o], weights[1, i, o]
            re = re + (a * w - b * v)
            im = im + (a * v + b * w)
        mixed_re.append(re)
        mixed_im.append(im)
    term = synthesise(
        jnp.concatenate(mixed_re, 0),
        jnp.concatenate(mixed_im, 0),
        phase[...],
        scaled_x[...],
        parts(plane),
    )
    for o in range(C):
        s = term[o] + local[o]
        bell = jnp.exp2(s * s * (-1.0 / math.log(2.0)))
        up[o] = cotangent[o] * ((1.0 + lax.erf(s)) + s * (2.0 / math.sqrt(math.pi)) * bell)
    analyse(lambda c: up[c], phase[...], parts(forward_x), plane, out)


def turned(modes):
    shape = (MODES, MODES)
    source, target = [lax.broadcasted_iota(jnp.int32, shape, axis) for axis in range(2)]
    wanted = target // 128 * 128 + (8 - target % 128 // K) % 8 * K + target % K
    order = (source == wanted).astype(jnp.bfloat16)
    high, rest = split_off(modes.reshape(ROWS, MODES))
    middle, rest = split_off(rest)
    total = 0.0
    for part in (rest.astype(jnp.bfloat16), middle, high):
        total = total + jnp.dot(part, order, preferred_element_type=jnp.float32)
    return total


def split_off(value):
    high = value.astype(jnp.bfloat16)
    return high, value - high.astype(jnp.float32)


def slabs(rows, start):
    half = rows[:, start : start + 128]
    return [
        pltpu.roll(jnp.broadcast_to(half[k : k + 1], (8, 128)), 0, 1, stride=K, stride_axis=0)
        for k in range(2 * C)
    ]


def backward_kernel(
    modes,
    back,
    weights,
    up,
    point,
    phase,
    inverse_x,
    plane,
    grad_fields,
    grad_spectral,
    cells,
    stored,
    sent,
):
    copies = []

    def send(source, target):
        copies.append(pltpu.make_async_copy(source, target, sent.at[len(copies)]))
        copies[-1].start()

    def one_wave(p):
        factor = (0.5 if p == 0 else 1.0) / float(N) ** 3
        first, second = [v[p * 2 * C : (p + 1) * 2 * C] for v in (modes_turned, back_turned)]
        second = second * factor
        for half in range(2):
            u, h = slabs(first, half * 128), slabs(second, half * 128)
            for i in range(C):
                for o in range(C):
                    re = u[i] * h[o] + u[C + i] * h[C + o]
                    im = u[i] * h[C + o] - u[C + i] * h[o]
                    stored[0, i, o, p, half * 8 : half * 8 + 8, :] = re[:, :K]
                    stored[1, i, o, p, half * 8 : half * 8 + 8, :] = im[:, :K]

    modes_turned, back_turned = turned(modes[...]), turned(back[...])
    for p in range(K):
        one_wave(p)
        if p % 4 == 3:
            some = pl.ds(p - 3, 4)
            send(stored.at[:, :, :, some], grad_spectral.at[:, :, :, some])
    adjoint_re, adjoint_im = [], []
    for i in range(C):
        re = im = 0.0
        for o in range(C):
            a, b = back[:, o, :], back[:, C + o, :]
            w, v = weights[0, i, o], weights[1, i, o]
            re = re + (a * w + b * v)
            im = im + (b * w - a * v)
        adjoint_re.append(re)
        adjoint_im.append(im)
    term = synthesise(
        jnp.concatenate(adjoint_re, 0),
        jnp.concatenate(adjoint_im, 0),
        phase[...],
        inverse_x[...],
        parts(plane),
    )
    for i in range(C):
        total = term[i]
        for o in range(C):
            total = total + (point[i, o] * 0.5) * up[o]
        cells[i] = total
        send(cells.at[i], grad_fields.at[i])
    for copy in copies:
        copy.wait()


def position_phase():
    lane = jnp.arange(MODES, dtype=jnp.int32)
    steps = (lane // K) * lax.axis_index("row") + (lane % K) * lax.axis_index("col")
    angle = (steps % K).astype(jnp.float32) * (2.0 * math.pi / K)
    return jnp.stack([jnp.cos(angle), -jnp.sin(angle)], 0)


def near(value):
    return pltpu.with_memory_space_constraint(value, pltpu.VMEM)


def far(value):
    return pltpu.with_memory_space_constraint(value, pltpu.HBM)


def near_out(shape, dtype=jnp.float32):
    return pltpu.VMEM(shape, dtype)


def groups():
    index = np.arange(256).reshape(2, 8, 4, 2, 2)
    index[0] = index[0, :, :, ::-1]
    index = index[::-1, [4, 5, 3, 6, 2, 7, 1, 0]][:, :, [2, 3, 1, 0], :, ::-1]
    index = index.reshape(K, K)
    return index.tolist(), index.T.tolist()


def swap(pieces, members):
    return lax.all_to_all(
        pieces, ("row", "col"), 0, 0, tiled=True, axis_index_groups=members
    )


def call(kernel, out_shape, in_specs, scratch_shapes=(), **more):
    where = [VMEM if not isinstance(o, jax.ShapeDtypeStruct) else HBM for o in out_shape]
    return pl.pallas_call(
        kernel,
        out_shape=tuple(out_shape),
        in_specs=in_specs,
        out_specs=tuple(where),
        scratch_shapes=scratch_shapes,
        compiler_params=PARAMS,
        **more,
    )


def total_modes(partial):
    shape = (K, 2 * C, MODES)
    near_by, alike = groups()
    pieces = near(swap(partial, near_by))
    (pieces,) = call(spread_kernel, [near_out(shape)], [VMEM])(pieces)
    pieces = near(swap(pieces, alike))
    (pieces,) = call(spread_kernel, [near_out(shape)], [VMEM])(pieces)
    return near(swap(pieces, near_by))


def per_device(fields, cotangent, spec_weights, point_weights, bias):
    forward_x, scaled_x, inverse_x, plane = [jnp.asarray(t) for t in tables()]
    shape = fields.shape
    cells = (C, CELLS, N)
    phase = near(position_phase())
    partial, fields, forward_x, plane = call(
        analysis_kernel,
        [
            near_out((K, 2 * C, MODES)),
            near_out(cells),
            near_out(forward_x.shape, jnp.bfloat16),
            near_out(plane.shape, jnp.bfloat16),
        ],
        [HBM] * 3 + [VMEM],
        [pltpu.SemaphoreType.DMA((C + 2,))],
    )(far(fields.reshape(cells)), far(forward_x), far(plane), phase)
    partial, cotangent = lax.optimization_barrier((partial, cotangent))
    fields, cotangent, forward_x, scaled_x, inverse_x, plane = [
        near(v)
        for v in (fields, cotangent.reshape(cells), forward_x, scaled_x, inverse_x, plane)
    ]
    weights = near(spec_weights.reshape(2, C, C, K, MODES))
    modes = total_modes(partial)
    (local,) = call(
        local_kernel, [near_out(cells)], [VMEM] + [SMEM] * 2, input_output_aliases={0: 0}
    )(fields, point_weights, bias)
    upstream, partial = call(
        forward_kernel,
        [near_out(cells), near_out((K, 2 * C, MODES))],
        [VMEM] * 8,
    )(modes, weights, near(local), cotangent, phase, forward_x, scaled_x, plane)
    back = total_modes(partial)
    grad_fields, grad_spectral = call(
        backward_kernel,
        [
            jax.ShapeDtypeStruct(cells, jnp.float32),
            jax.ShapeDtypeStruct((2, C, C, K, K, K), jnp.float32),
        ],
        [VMEM] * 4 + [SMEM] + [VMEM] * 3,
        [
            pltpu.VMEM(cells, jnp.float32),
            pltpu.VMEM((2, C, C, K, K, K), jnp.float32),
            pltpu.SemaphoreType.DMA((8,)),
        ],
    )(modes, back, weights, near(upstream), point_weights, phase, inverse_x, plane)
    return grad_fields.reshape(shape), grad_spectral


def solution(mesh):
    placed = P(None, None, "row", "col", None)
    return jax.shard_map(
        per_device,
        mesh=mesh,
        in_specs=(placed, placed, P(), P(), P()),
        out_specs=(placed, P()),
        check_vma=False,
    )
```

```python
import functools
import math

import jax
import jax.numpy as jnp
import numpy as np
from jax import lax
from jax.experimental import pallas as pl
from jax.experimental.pallas import tpu as pltpu
from jax.sharding import PartitionSpec as P

C = 4
N = 256
K = 16
LOCAL = 16
CELLS = LOCAL * LOCAL
MODES = K * K
ROWS = 2 * C * K
HALF_ROOT = math.sqrt(0.5)

VMEM = pl.BlockSpec(memory_space=pltpu.VMEM)
HBM = pl.BlockSpec(memory_space=pltpu.HBM)
SMEM = pl.BlockSpec(memory_space=pltpu.SMEM)
PARAMS = pltpu.CompilerParams(vmem_limit_bytes=24 << 20)
NT = (((1,), (1,)), ((), ()))
NN = (((1,), (0,)), ((), ()))
TN = (((0,), (0,)), ((), ()))


def two_parts(table):
    high = np.asarray(table, jnp.bfloat16)
    low = np.asarray(table - np.asarray(high, np.float64), jnp.bfloat16)
    return np.stack([high, low])


def joined(table):
    high, low = two_parts(table)
    return np.concatenate([high, high, low], 0)


def signed_waves():
    index = np.arange(K)
    return np.where(index < K // 2, index, index - K)


def tables():
    angle = 2.0 * np.pi / N * (np.arange(K)[:, None] * np.arange(N)[None, :] % N)
    forward_x = np.concatenate([np.cos(angle), -np.sin(angle)], 0)
    weighting = np.where(np.arange(K) == 0, 1.0, 2.0)[:, None] / float(N) ** 3
    inverse_x = np.concatenate([np.cos(angle) * weighting, -np.sin(angle) * weighting], 0)
    one = np.arange(LOCAL)[:, None] * signed_waves()[None, :]
    both = one[:, None, :, None] + one[None, :, None, :]
    angle = 2.0 * np.pi / N * (both.reshape(CELLS, MODES) % N)
    plane = np.concatenate([np.cos(angle), -np.sin(angle)], 1)
    scaled_x, inverse_x = joined(inverse_x * np.sqrt(0.5)), joined(inverse_x * 0.5)
    return two_parts(forward_x), scaled_x, inverse_x, two_parts(plane)


def split(value):
    high = value.astype(jnp.bfloat16)
    low = (value - high.astype(jnp.float32)).astype(jnp.bfloat16)
    return high, low


def dot_of(dims):
    return functools.partial(
        lax.dot_general, dimension_numbers=dims, preferred_element_type=jnp.float32
    )


def dot3(left, right, dims):
    dot = dot_of(dims)
    rows = left[0].shape[0]
    both = dot(jnp.concatenate(left, 0), right[0])
    return both[:rows] + (dot(left[0], right[1]) + both[rows:])


def analyse(channel, phase, forward_x, plane, out, ready=None):
    real, imag = [], []
    for c in range(C):
        along_x = dot3(forward_x, split(channel(c)), NT)
        real.append(along_x[:K])
        imag.append(along_x[K:])
    if ready is not None:
        ready()
    both = dot3(split(jnp.concatenate(real + imag, 0)), parts(plane), NN)
    half = ROWS // 2
    part_re = both[:half, :MODES] - both[half:, MODES:]
    part_im = both[:half, MODES:] + both[half:, :MODES]
    cosine, sine = phase[0:1, :], phase[1:2, :]
    for t, part in enumerate(
        (part_re * cosine - part_im * sine, part_re * sine + part_im * cosine)
    ):
        for c in range(C):
            out[:, t * C + c, :] = part[c * K : (c + 1) * K]


def synthesise(modes_re, modes_im, phase, inverse_x, plane):
    cosine, sine = phase[0:1, :], phase[1:2, :]
    here_re = modes_re * cosine + modes_im * sine
    here_im = modes_im * cosine - modes_re * sine
    left = jnp.concatenate(
        [jnp.concatenate([here_re, here_im], 1), jnp.concatenate([here_im, -here_re], 1)], 0
    )
    lines = dot3(split(left), plane, NT)
    half = ROWS // 2
    out = []
    for c in range(C):
        pair = jnp.concatenate([lines[c * K : (c + 1) * K], lines[half + c * K :][:K]], 0)
        high, low = split(pair)
        out.append(dot_of(TN)(jnp.concatenate([high, low, high], 0), inverse_x))
    return out


def parts(ref):
    return ref[0], ref[1]


def analysis_kernel(fields, forward_x, plane, phase, out, cells, lines, square, arrived):
    table = pltpu.make_async_copy(forward_x, lines, arrived.at[C])
    table.start()
    copies = [
        pltpu.make_async_copy(fields.at[c], cells.at[c], arrived.at[c]) for c in range(C)
    ]
    for copy in copies:
        copy.start()
    second = pltpu.make_async_copy(plane, square, arrived.at[C + 1])
    second.start()
    table.wait()

    def channel(c):
        copies[c].wait()
        return cells[c]

    analyse(channel, phase[...], parts(lines), square, out, second.wait)


def spread_kernel(pieces, out):
    total = jnp.sum(pieces[...], axis=0)
    out[...] = jnp.broadcast_to(total[None], out.shape)


def local_kernel(fields, point, bias, out):
    del fields
    for start in range(0, CELLS, 8):
        cells = [out[i, start : start + 8] for i in range(C)]
        for o in range(C):
            total = bias[o] * HALF_ROOT
            for i in range(C):
                total = total + (point[i, o] * HALF_ROOT) * cells[i]
            out[o, start : start + 8] = total


def forward_kernel(
    modes, weights, local, cotangent, phase, forward_x, scaled_x, plane, up, out
):
    mixed_re, mixed_im = [], []
    for o in range(C):
        re = im = 0.0
        for i in range(C):
            a, b = modes[:, i, :], modes[:, C + i, :]
            w, v = weights[0, i, o], weights[1, i, o]
            re = re + (a * w - b * v)
            im = im + (a * v + b * w)
        mixed_re.append(re)
        mixed_im.append(im)
    term = synthesise(
        jnp.concatenate(mixed_re, 0),
        jnp.concatenate(mixed_im, 0),
        phase[...],
        scaled_x[...],
        parts(plane),
    )
    for o in range(C):
        s = term[o] + local[o]
        bell = jnp.exp2(s * s * (-1.0 / math.log(2.0)))
        up[o] = cotangent[o] * ((1.0 + lax.erf(s)) + s * (2.0 / math.sqrt(math.pi)) * bell)
    analyse(lambda c: up[c], phase[...], parts(forward_x), plane, out)


def turned(modes):
    shape = (MODES, MODES)
    source, target = [lax.broadcasted_iota(jnp.int32, shape, axis) for axis in range(2)]
    wanted = target // 128 * 128 + (8 - target % 128 // K) % 8 * K + target % K
    order = (source == wanted).astype(jnp.bfloat16)
    high, rest = split_off(modes.reshape(ROWS, MODES))
    middle, rest = split_off(rest)
    total = 0.0
    for part in (rest.astype(jnp.bfloat16), middle, high):
        total = total + jnp.dot(part, order, preferred_element_type=jnp.float32)
    return total


def split_off(value):
    high = value.astype(jnp.bfloat16)
    return high, value - high.astype(jnp.float32)


def slabs(rows, start):
    half = rows[:, start : start + 128]
    return [
        pltpu.roll(jnp.broadcast_to(half[k : k + 1], (8, 128)), 0, 1, stride=K, stride_axis=0)
        for k in range(2 * C)
    ]


def backward_kernel(
    modes,
    back,
    weights,
    up,
    point,
    phase,
    inverse_x,
    plane,
    grad_fields,
    grad_spectral,
    cells,
    stored,
    sent,
):
    copies = []

    def send(source, target):
        copies.append(pltpu.make_async_copy(source, target, sent.at[len(copies)]))
        copies[-1].start()

    def one_wave(p):
        factor = (0.5 if p == 0 else 1.0) / float(N) ** 3
        first, second = [v[p * 2 * C : (p + 1) * 2 * C] for v in (modes_turned, back_turned)]
        second = second * factor
        for half in range(2):
            u, h = slabs(first, half * 128), slabs(second, half * 128)
            for i in range(C):
                for o in range(C):
                    re = u[i] * h[o] + u[C + i] * h[C + o]
                    im = u[i] * h[C + o] - u[C + i] * h[o]
                    stored[0, i, o, p, half * 8 : half * 8 + 8, :] = re[:, :K]
                    stored[1, i, o, p, half * 8 : half * 8 + 8, :] = im[:, :K]

    modes_turned, back_turned = turned(modes[...]), turned(back[...])
    for p in range(K):
        one_wave(p)
        if p % 4 == 3:
            some = pl.ds(p - 3, 4)
            send(stored.at[:, :, :, some], grad_spectral.at[:, :, :, some])
    adjoint_re, adjoint_im = [], []
    for i in range(C):
        re = im = 0.0
        for o in range(C):
            a, b = back[:, o, :], back[:, C + o, :]
            w, v = weights[0, i, o], weights[1, i, o]
            re = re + (a * w + b * v)
            im = im + (b * w - a * v)
        adjoint_re.append(re)
        adjoint_im.append(im)
    term = synthesise(
        jnp.concatenate(adjoint_re, 0),
        jnp.concatenate(adjoint_im, 0),
        phase[...],
        inverse_x[...],
        parts(plane),
    )
    for i in range(C):
        total = term[i]
        for o in range(C):
            total = total + (point[i, o] * 0.5) * up[o]
        cells[i] = total
        send(cells.at[i], grad_fields.at[i])
    for copy in copies:
        copy.wait()


def position_phase():
    lane = jnp.arange(MODES, dtype=jnp.int32)
    steps = (lane // K) * lax.axis_index("row") + (lane % K) * lax.axis_index("col")
    angle = (steps % K).astype(jnp.float32) * (2.0 * math.pi / K)
    return jnp.stack([jnp.cos(angle), -jnp.sin(angle)], 0)


def near(value):
    return pltpu.with_memory_space_constraint(value, pltpu.VMEM)


def far(value):
    return pltpu.with_memory_space_constraint(value, pltpu.HBM)


def near_out(shape, dtype=jnp.float32):
    return pltpu.VMEM(shape, dtype)


def groups():
    index = np.arange(256).reshape(2, 8, 4, 2, 2)
    index[0] = index[0, :, :, ::-1]
    index = index[::-1, [4, 5, 3, 6, 2, 7, 1, 0]][:, :, [2, 3, 1, 0], :, ::-1]
    index = index.reshape(K, K)
    return index.tolist(), index.T.tolist()


def swap(pieces, members):
    return lax.all_to_all(
        pieces, ("row", "col"), 0, 0, tiled=True, axis_index_groups=members
    )


def call(kernel, out_shape, in_specs, scratch_shapes=(), **more):
    where = [VMEM if not isinstance(o, jax.ShapeDtypeStruct) else HBM for o in out_shape]
    return pl.pallas_call(
        kernel,
        out_shape=tuple(out_shape),
        in_specs=in_specs,
        out_specs=tuple(where),
        scratch_shapes=scratch_shapes,
        compiler_params=PARAMS,
        **more,
    )


def total_modes(partial, *beside):
    shape = (K, 2 * C, MODES)
    near_by, alike = groups()
    pieces = near(swap(partial, near_by))
    (pieces,) = call(spread_kernel, [near_out(shape)], [VMEM])(pieces)
    pieces, *beside = lax.optimization_barrier((swap(pieces, alike), *beside))
    pieces = near(pieces)
    (pieces,) = call(spread_kernel, [near_out(shape)], [VMEM])(pieces)
    return near(swap(pieces, near_by)), *beside


def per_device(fields, cotangent, spec_weights, point_weights, bias):
    forward_x, scaled_x, inverse_x, plane = [jnp.asarray(t) for t in tables()]
    shape = fields.shape
    cells = (C, CELLS, N)
    phase = near(position_phase())
    partial, fields, forward_x, plane = call(
        analysis_kernel,
        [
            near_out((K, 2 * C, MODES)),
            near_out(cells),
            near_out(forward_x.shape, jnp.bfloat16),
            near_out(plane.shape, jnp.bfloat16),
        ],
        [HBM] * 3 + [VMEM],
        [pltpu.SemaphoreType.DMA((C + 2,))],
    )(far(fields.reshape(cells)), far(forward_x), far(plane), phase)
    partial, cotangent = lax.optimization_barrier((partial, cotangent))
    fields, cotangent, forward_x, scaled_x, inverse_x, plane = [
        near(v)
        for v in (fields, cotangent.reshape(cells), forward_x, scaled_x, inverse_x, plane)
    ]
    weights = spec_weights.reshape(2, C, C, K, MODES)
    (local,) = call(
        local_kernel, [near_out(cells)], [VMEM] + [SMEM] * 2, input_output_aliases={0: 0}
    )(fields, point_weights, bias)
    modes, weights, local = total_modes(partial, weights, local)
    weights = near(weights)
    upstream, partial = call(
        forward_kernel,
        [near_out(cells), near_out((K, 2 * C, MODES))],
        [VMEM] * 8,
    )(modes, weights, near(local), cotangent, phase, forward_x, scaled_x, plane)
    (back,) = total_modes(partial)
    grad_fields, grad_spectral = call(
        backward_kernel,
        [
            jax.ShapeDtypeStruct(cells, jnp.float32),
            jax.ShapeDtypeStruct((2, C, C, K, K, K), jnp.float32),
        ],
        [VMEM] * 4 + [SMEM] + [VMEM] * 3,
        [
            pltpu.VMEM(cells, jnp.float32),
            pltpu.VMEM((2, C, C, K, K, K), jnp.float32),
            pltpu.SemaphoreType.DMA((8,)),
        ],
    )(modes, back, weights, near(upstream), point_weights, phase, inverse_x, plane)
    return grad_fields.reshape(shape), grad_spectral


def solution(mesh):
    placed = P(None, None, "row", "col", None)
    return jax.shard_map(
        per_device,
        mesh=mesh,
        in_specs=(placed, placed, P(), P(), P()),
        out_specs=(placed, P()),
        check_vma=False,
    )
```

```python
import functools
import math

import jax
import jax.numpy as jnp
import numpy as np
from jax import lax
from jax.experimental import pallas as pl
from jax.experimental.pallas import tpu as pltpu
from jax.sharding import PartitionSpec as P

C = 4
N = 256
K = 16
LOCAL = 16
CELLS = LOCAL * LOCAL
MODES = K * K
ROWS = 2 * C * K
HALF_ROOT = math.sqrt(0.5)

VMEM = pl.BlockSpec(memory_space=pltpu.VMEM)
HBM = pl.BlockSpec(memory_space=pltpu.HBM)
SMEM = pl.BlockSpec(memory_space=pltpu.SMEM)
PARAMS = pltpu.CompilerParams(vmem_limit_bytes=24 << 20)
NT = (((1,), (1,)), ((), ()))
NN = (((1,), (0,)), ((), ()))
TN = (((0,), (0,)), ((), ()))


def two_parts(table):
    high = np.asarray(table, jnp.bfloat16)
    low = np.asarray(table - np.asarray(high, np.float64), jnp.bfloat16)
    return np.stack([high, low])


def joined(table):
    high, low = two_parts(table)
    return np.concatenate([high, high, low], 0)


def signed_waves():
    index = np.arange(K)
    return np.where(index < K // 2, index, index - K)


def tables():
    angle = 2.0 * np.pi / N * (np.arange(K)[:, None] * np.arange(N)[None, :] % N)
    forward_x = np.concatenate([np.cos(angle), -np.sin(angle)], 0)
    weighting = np.where(np.arange(K) == 0, 1.0, 2.0)[:, None] / float(N) ** 3
    inverse_x = np.concatenate([np.cos(angle) * weighting, -np.sin(angle) * weighting], 0)
    one = np.arange(LOCAL)[:, None] * signed_waves()[None, :]
    both = one[:, None, :, None] + one[None, :, None, :]
    angle = 2.0 * np.pi / N * (both.reshape(CELLS, MODES) % N)
    plane = np.concatenate([np.cos(angle), -np.sin(angle)], 1)
    scaled_x, inverse_x = joined(inverse_x * np.sqrt(0.5)), joined(inverse_x * 0.5)
    return two_parts(forward_x), scaled_x, inverse_x, two_parts(plane)


def split(value):
    high = value.astype(jnp.bfloat16)
    low = (value - high.astype(jnp.float32)).astype(jnp.bfloat16)
    return high, low


def dot_of(dims):
    return functools.partial(
        lax.dot_general, dimension_numbers=dims, preferred_element_type=jnp.float32
    )


def dot3(left, right, dims):
    dot = dot_of(dims)
    rows = left[0].shape[0]
    both = dot(jnp.concatenate(left, 0), right[0])
    return both[:rows] + (dot(left[0], right[1]) + both[rows:])


def analyse(channel, phase, forward_x, plane, out, ready=None):
    real, imag = [], []
    for c in range(C):
        along_x = dot3(forward_x, split(channel(c)), NT)
        real.append(along_x[:K])
        imag.append(along_x[K:])
    if ready is not None:
        ready()
    both = dot3(split(jnp.concatenate(real + imag, 0)), parts(plane), NN)
    half = ROWS // 2
    part_re = both[:half, :MODES] - both[half:, MODES:]
    part_im = both[:half, MODES:] + both[half:, :MODES]
    cosine, sine = phase[0:1, :], phase[1:2, :]
    for t, part in enumerate(
        (part_re * cosine - part_im * sine, part_re * sine + part_im * cosine)
    ):
        for c in range(C):
            out[:, t * C + c, :] = part[c * K : (c + 1) * K]


def synthesise(modes_re, modes_im, phase, inverse_x, plane):
    cosine, sine = phase[0:1, :], phase[1:2, :]
    here_re = modes_re * cosine + modes_im * sine
    here_im = modes_im * cosine - modes_re * sine
    left = jnp.concatenate(
        [jnp.concatenate([here_re, here_im], 1), jnp.concatenate([here_im, -here_re], 1)], 0
    )
    lines = dot3(split(left), plane, NT)
    half = ROWS // 2
    out = []
    for c in range(C):
        pair = jnp.concatenate([lines[c * K : (c + 1) * K], lines[half + c * K :][:K]], 0)
        high, low = split(pair)
        out.append(dot_of(TN)(jnp.concatenate([high, low, high], 0), inverse_x))
    return out


def parts(ref):
    return ref[0], ref[1]


def analysis_kernel(fields, forward_x, plane, phase, out, cells, lines, square, arrived):
    table = pltpu.make_async_copy(forward_x, lines, arrived.at[C])
    table.start()
    copies = [
        pltpu.make_async_copy(fields.at[c], cells.at[c], arrived.at[c]) for c in range(C)
    ]
    for copy in copies:
        copy.start()
    second = pltpu.make_async_copy(plane, square, arrived.at[C + 1])
    second.start()
    table.wait()

    def channel(c):
        if c % 2 == 0:
            copies[c].wait()
            copies[c + 1].wait()
        return cells[c]

    analyse(channel, phase[...], parts(lines), square, out, second.wait)


def spread_kernel(pieces, out):
    total = jnp.sum(pieces[...], axis=0)
    out[...] = jnp.broadcast_to(total[None], out.shape)


def local_kernel(fields, point, bias, out):
    del fields
    for start in range(0, CELLS, 8):
        cells = [out[i, start : start + 8] for i in range(C)]
        for o in range(C):
            total = bias[o] * HALF_ROOT
            for i in range(C):
                total = total + (point[i, o] * HALF_ROOT) * cells[i]
            out[o, start : start + 8] = total


def forward_kernel(
    modes, weights, local, cotangent, phase, forward_x, scaled_x, plane, up, out
):
    mixed_re, mixed_im = [], []
    for o in range(C):
        re = im = 0.0
        for i in range(C):
            a, b = modes[:, i, :], modes[:, C + i, :]
            w, v = weights[0, i, o], weights[1, i, o]
            re = re + (a * w - b * v)
            im = im + (a * v + b * w)
        mixed_re.append(re)
        mixed_im.append(im)
    term = synthesise(
        jnp.concatenate(mixed_re, 0),
        jnp.concatenate(mixed_im, 0),
        phase[...],
        scaled_x[...],
        parts(plane),
    )
    for o in range(C):
        s = term[o] + local[o]
        bell = jnp.exp2(s * s * (-1.0 / math.log(2.0)))
        up[o] = cotangent[o] * ((1.0 + lax.erf(s)) + s * (2.0 / math.sqrt(math.pi)) * bell)
    analyse(lambda c: up[c], phase[...], parts(forward_x), plane, out)


def turned(modes):
    shape = (MODES, MODES)
    source, target = [lax.broadcasted_iota(jnp.int32, shape, axis) for axis in range(2)]
    wanted = target // 128 * 128 + (8 - target % 128 // K) % 8 * K + target % K
    order = (source == wanted).astype(jnp.bfloat16)
    high, rest = split_off(modes.reshape(ROWS, MODES))
    middle, rest = split_off(rest)
    total = 0.0
    for part in (rest.astype(jnp.bfloat16), middle, high):
        total = total + jnp.dot(part, order, preferred_element_type=jnp.float32)
    return total


def split_off(value):
    high = value.astype(jnp.bfloat16)
    return high, value - high.astype(jnp.float32)


def slabs(rows, start):
    half = rows[:, start : start + 128]
    return [
        pltpu.roll(jnp.broadcast_to(half[k : k + 1], (8, 128)), 0, 1, stride=K, stride_axis=0)
        for k in range(2 * C)
    ]


def backward_kernel(
    modes,
    back,
    weights,
    up,
    point,
    phase,
    inverse_x,
    plane,
    grad_fields,
    grad_spectral,
    cells,
    stored,
    sent,
):
    copies = []

    def send(source, target):
        copies.append(pltpu.make_async_copy(source, target, sent.at[len(copies)]))
        copies[-1].start()

    def one_wave(p):
        factor = (0.5 if p == 0 else 1.0) / float(N) ** 3
        first, second = [v[p * 2 * C : (p + 1) * 2 * C] for v in (modes_turned, back_turned)]
        second = second * factor
        for half in range(2):
            u, h = slabs(first, half * 128), slabs(second, half * 128)
            for i in range(C):
                for o in range(C):
                    re = u[i] * h[o] + u[C + i] * h[C + o]
                    im = u[i] * h[C + o] - u[C + i] * h[o]
                    stored[0, i, o, p, half * 8 : half * 8 + 8, :] = re[:, :K]
                    stored[1, i, o, p, half * 8 : half * 8 + 8, :] = im[:, :K]

    modes_turned, back_turned = turned(modes[...]), turned(back[...])
    for p in range(K):
        one_wave(p)
        if p % 2 == 1:
            some = pl.ds(p - 1, 2)
            send(stored.at[:, :, :, some], grad_spectral.at[:, :, :, some])
    adjoint_re, adjoint_im = [], []
    for i in range(C):
        re = im = 0.0
        for o in range(C):
            a, b = back[:, o, :], back[:, C + o, :]
            w, v = weights[0, i, o], weights[1, i, o]
            re = re + (a * w + b * v)
            im = im + (b * w - a * v)
        adjoint_re.append(re)
        adjoint_im.append(im)
    term = synthesise(
        jnp.concatenate(adjoint_re, 0),
        jnp.concatenate(adjoint_im, 0),
        phase[...],
        inverse_x[...],
        parts(plane),
    )
    for i in range(C):
        total = term[i]
        for o in range(C):
            total = total + (point[i, o] * 0.5) * up[o]
        cells[i] = total
        send(cells.at[i], grad_fields.at[i])
    for copy in copies:
        copy.wait()


def position_phase():
    lane = jnp.arange(MODES, dtype=jnp.int32)
    steps = (lane // K) * lax.axis_index("row") + (lane % K) * lax.axis_index("col")
    angle = (steps % K).astype(jnp.float32) * (2.0 * math.pi / K)
    return jnp.stack([jnp.cos(angle), -jnp.sin(angle)], 0)


def near(value):
    return pltpu.with_memory_space_constraint(value, pltpu.VMEM)


def far(value):
    return pltpu.with_memory_space_constraint(value, pltpu.HBM)


def near_out(shape, dtype=jnp.float32):
    return pltpu.VMEM(shape, dtype)


def groups():
    index = np.arange(256).reshape(2, 8, 4, 2, 2)
    index[0] = index[0, :, :, ::-1]
    index = index[::-1, [4, 5, 3, 6, 2, 7, 1, 0]][:, :, [2, 3, 1, 0], :, ::-1]
    index = index.reshape(K, K)
    return index.tolist(), index.T.tolist()


def swap(pieces, members):
    return lax.all_to_all(
        pieces, ("row", "col"), 0, 0, tiled=True, axis_index_groups=members
    )


def call(kernel, out_shape, in_specs, scratch_shapes=(), **more):
    where = [VMEM if not isinstance(o, jax.ShapeDtypeStruct) else HBM for o in out_shape]
    return pl.pallas_call(
        kernel,
        out_shape=tuple(out_shape),
        in_specs=in_specs,
        out_specs=tuple(where),
        scratch_shapes=scratch_shapes,
        compiler_params=PARAMS,
        **more,
    )


def total_modes(partial, *beside):
    shape = (K, 2 * C, MODES)
    near_by, alike = groups()
    pieces = near(swap(partial, near_by))
    (pieces,) = call(spread_kernel, [near_out(shape)], [VMEM])(pieces)
    pieces, *beside = lax.optimization_barrier((swap(pieces, alike), *beside))
    pieces = near(pieces)
    (pieces,) = call(spread_kernel, [near_out(shape)], [VMEM])(pieces)
    return near(swap(pieces, near_by)), *beside


def per_device(fields, cotangent, spec_weights, point_weights, bias):
    forward_x, scaled_x, inverse_x, plane = [jnp.asarray(t) for t in tables()]
    shape = fields.shape
    cells = (C, CELLS, N)
    phase = near(position_phase())
    partial, fields, forward_x, plane = call(
        analysis_kernel,
        [
            near_out((K, 2 * C, MODES)),
            near_out(cells),
            near_out(forward_x.shape, jnp.bfloat16),
            near_out(plane.shape, jnp.bfloat16),
        ],
        [HBM] * 3 + [VMEM],
        [pltpu.SemaphoreType.DMA((C + 2,))],
    )(far(fields.reshape(cells)), far(forward_x), far(plane), phase)
    partial, cotangent = lax.optimization_barrier((partial, cotangent))
    fields, cotangent, forward_x, scaled_x, inverse_x, plane = [
        near(v)
        for v in (fields, cotangent.reshape(cells), forward_x, scaled_x, inverse_x, plane)
    ]
    weights = spec_weights.reshape(2, C, C, K, MODES)
    (local,) = call(
        local_kernel, [near_out(cells)], [VMEM] + [SMEM] * 2, input_output_aliases={0: 0}
    )(fields, point_weights, bias)
    modes, weights, local = total_modes(partial, weights, local)
    weights = near(weights)
    upstream, partial = call(
        forward_kernel,
        [near_out(cells), near_out((K, 2 * C, MODES))],
        [VMEM] * 8,
    )(modes, weights, near(local), cotangent, phase, forward_x, scaled_x, plane)
    (back,) = total_modes(partial)
    grad_fields, grad_spectral = call(
        backward_kernel,
        [
            jax.ShapeDtypeStruct(cells, jnp.float32),
            jax.ShapeDtypeStruct((2, C, C, K, K, K), jnp.float32),
        ],
        [VMEM] * 4 + [SMEM] + [VMEM] * 3,
        [
            pltpu.VMEM(cells, jnp.float32),
            pltpu.VMEM((2, C, C, K, K, K), jnp.float32),
            pltpu.SemaphoreType.DMA((12,)),
        ],
    )(modes, back, weights, near(upstream), point_weights, phase, inverse_x, plane)
    return grad_fields.reshape(shape), grad_spectral


def solution(mesh):
    placed = P(None, None, "row", "col", None)
    return jax.shard_map(
        per_device,
        mesh=mesh,
        in_specs=(placed, placed, P(), P(), P()),
        out_specs=(placed, P()),
        check_vma=False,
    )
```

```python
import functools
import math

import jax
import jax.numpy as jnp
import numpy as np
from jax import lax
from jax.experimental import pallas as pl
from jax.experimental.pallas import tpu as pltpu
from jax.sharding import PartitionSpec as P

C = 4
N = 256
K = 16
LOCAL = 16
CELLS = LOCAL * LOCAL
MODES = K * K
ROWS = 2 * C * K
HALF_ROOT = math.sqrt(0.5)

VMEM = pl.BlockSpec(memory_space=pltpu.VMEM)
HBM = pl.BlockSpec(memory_space=pltpu.HBM)
SMEM = pl.BlockSpec(memory_space=pltpu.SMEM)
PARAMS = pltpu.CompilerParams(vmem_limit_bytes=24 << 20)
NT = (((1,), (1,)), ((), ()))
NN = (((1,), (0,)), ((), ()))
TN = (((0,), (0,)), ((), ()))


def two_parts(table):
    high = np.asarray(table, jnp.bfloat16)
    low = np.asarray(table - np.asarray(high, np.float64), jnp.bfloat16)
    return np.stack([high, low])


def joined(table):
    high, low = two_parts(table)
    return np.concatenate([high, high, low], 0)


def signed_waves():
    index = np.arange(K)
    return np.where(index < K // 2, index, index - K)


def tables():
    angle = 2.0 * np.pi / N * (np.arange(K)[:, None] * np.arange(N)[None, :] % N)
    forward_x = np.concatenate([np.cos(angle), -np.sin(angle)], 0)
    weighting = np.where(np.arange(K) == 0, 1.0, 2.0)[:, None] / float(N) ** 3
    inverse_x = np.concatenate([np.cos(angle) * weighting, -np.sin(angle) * weighting], 0)
    one = np.arange(LOCAL)[:, None] * signed_waves()[None, :]
    both = one[:, None, :, None] + one[None, :, None, :]
    angle = 2.0 * np.pi / N * (both.reshape(CELLS, MODES) % N)
    plane = np.concatenate([np.cos(angle), -np.sin(angle)], 1)
    scaled_x, inverse_x = joined(inverse_x * np.sqrt(0.5)), joined(inverse_x * 0.5)
    return two_parts(forward_x), scaled_x, inverse_x, two_parts(plane)


def split(value):
    high = value.astype(jnp.bfloat16)
    low = (value - high.astype(jnp.float32)).astype(jnp.bfloat16)
    return high, low


def dot_of(dims):
    return functools.partial(
        lax.dot_general, dimension_numbers=dims, preferred_element_type=jnp.float32
    )


def dot3(left, right, dims):
    dot = dot_of(dims)
    rows = left[0].shape[0]
    both = dot(jnp.concatenate(left, 0), right[0])
    return both[:rows] + (dot(left[0], right[1]) + both[rows:])


def analyse(channel, phase, forward_x, plane, out, ready=None):
    real, imag = [], []
    for c in range(C):
        along_x = dot3(forward_x, split(channel(c)), NT)
        real.append(along_x[:K])
        imag.append(along_x[K:])
    if ready is not None:
        ready()
    both = dot3(split(jnp.concatenate(real + imag, 0)), parts(plane), NN)
    half = ROWS // 2
    part_re = both[:half, :MODES] - both[half:, MODES:]
    part_im = both[:half, MODES:] + both[half:, :MODES]
    cosine, sine = phase[0:1, :], phase[1:2, :]
    for t, part in enumerate(
        (part_re * cosine - part_im * sine, part_re * sine + part_im * cosine)
    ):
        for c in range(C):
            out[:, t * C + c, :] = part[c * K : (c + 1) * K]


def synthesise(modes_re, modes_im, phase, inverse_x, plane):
    cosine, sine = phase[0:1, :], phase[1:2, :]
    here_re = modes_re * cosine + modes_im * sine
    here_im = modes_im * cosine - modes_re * sine
    left = jnp.concatenate(
        [jnp.concatenate([here_re, here_im], 1), jnp.concatenate([here_im, -here_re], 1)], 0
    )
    lines = dot3(split(left), plane, NT)
    half = ROWS // 2
    out = []
    for c in range(C):
        pair = jnp.concatenate([lines[c * K : (c + 1) * K], lines[half + c * K :][:K]], 0)
        high, low = split(pair)
        out.append(dot_of(TN)(jnp.concatenate([high, low, high], 0), inverse_x))
    return out


def parts(ref):
    return ref[0], ref[1]


def analysis_kernel(fields, forward_x, plane, out, cells, lines, square, phase, arrived):
    table = pltpu.make_async_copy(forward_x, lines, arrived.at[C])
    table.start()
    copies = [
        pltpu.make_async_copy(fields.at[c], cells.at[c], arrived.at[c]) for c in range(C)
    ]
    for copy in copies:
        copy.start()
    second = pltpu.make_async_copy(plane, square, arrived.at[C + 1])
    second.start()
    phase[...] = position_phase()
    table.wait()

    def channel(c):
        if c % 2 == 0:
            copies[c].wait()
            copies[c + 1].wait()
        return cells[c]

    analyse(channel, phase[...], parts(lines), square, out, second.wait)


def spread_kernel(pieces, out):
    total = jnp.sum(pieces[...], axis=0)
    out[...] = jnp.broadcast_to(total[None], out.shape)


def local_kernel(fields, point, bias, out):
    del fields
    for start in range(0, CELLS, 8):
        cells = [out[i, start : start + 8] for i in range(C)]
        for o in range(C):
            total = bias[o] * HALF_ROOT
            for i in range(C):
                total = total + (point[i, o] * HALF_ROOT) * cells[i]
            out[o, start : start + 8] = total


def forward_kernel(
    modes, weights, local, cotangent, phase, forward_x, scaled_x, plane, up, out
):
    mixed_re, mixed_im = [], []
    for o in range(C):
        re = im = 0.0
        for i in range(C):
            a, b = modes[:, i, :], modes[:, C + i, :]
            w, v = weights[0, i, o], weights[1, i, o]
            re = re + (a * w - b * v)
            im = im + (a * v + b * w)
        mixed_re.append(re)
        mixed_im.append(im)
    term = synthesise(
        jnp.concatenate(mixed_re, 0),
        jnp.concatenate(mixed_im, 0),
        phase[...],
        scaled_x[...],
        parts(plane),
    )
    for o in range(C):
        s = term[o] + local[o]
        bell = jnp.exp2(s * s * (-1.0 / math.log(2.0)))
        up[o] = cotangent[o] * ((1.0 + lax.erf(s)) + s * (2.0 / math.sqrt(math.pi)) * bell)
    analyse(lambda c: up[c], phase[...], parts(forward_x), plane, out)


def turned(modes):
    shape = (MODES, MODES)
    source, target = [lax.broadcasted_iota(jnp.int32, shape, axis) for axis in range(2)]
    wanted = target // 128 * 128 + (8 - target % 128 // K) % 8 * K + target % K
    order = (source == wanted).astype(jnp.bfloat16)
    high, rest = split_off(modes.reshape(ROWS, MODES))
    middle, rest = split_off(rest)
    total = 0.0
    for part in (rest.astype(jnp.bfloat16), middle, high):
        total = total + jnp.dot(part, order, preferred_element_type=jnp.float32)
    return total


def split_off(value):
    high = value.astype(jnp.bfloat16)
    return high, value - high.astype(jnp.float32)


def slabs(rows, start):
    half = rows[:, start : start + 128]
    return [
        pltpu.roll(jnp.broadcast_to(half[k : k + 1], (8, 128)), 0, 1, stride=K, stride_axis=0)
        for k in range(2 * C)
    ]


def backward_kernel(
    modes,
    back,
    weights,
    up,
    point,
    phase,
    inverse_x,
    plane,
    grad_fields,
    grad_spectral,
    cells,
    stored,
    sent,
):
    copies = []

    def send(source, target):
        copies.append(pltpu.make_async_copy(source, target, sent.at[len(copies)]))
        copies[-1].start()

    def one_wave(p):
        factor = (0.5 if p == 0 else 1.0) / float(N) ** 3
        first, second = [v[p * 2 * C : (p + 1) * 2 * C] for v in (modes_turned, back_turned)]
        second = second * factor
        for half in range(2):
            u, h = slabs(first, half * 128), slabs(second, half * 128)
            for i in range(C):
                for o in range(C):
                    re = u[i] * h[o] + u[C + i] * h[C + o]
                    im = u[i] * h[C + o] - u[C + i] * h[o]
                    stored[0, i, o, p, half * 8 : half * 8 + 8, :] = re[:, :K]
                    stored[1, i, o, p, half * 8 : half * 8 + 8, :] = im[:, :K]

    modes_turned, back_turned = turned(modes[...]), turned(back[...])
    for p in range(K):
        one_wave(p)
        if p % 2 == 1:
            some = pl.ds(p - 1, 2)
            send(stored.at[:, :, :, some], grad_spectral.at[:, :, :, some])
    adjoint_re, adjoint_im = [], []
    for i in range(C):
        re = im = 0.0
        for o in range(C):
            a, b = back[:, o, :], back[:, C + o, :]
            w, v = weights[0, i, o], weights[1, i, o]
            re = re + (a * w + b * v)
            im = im + (b * w - a * v)
        adjoint_re.append(re)
        adjoint_im.append(im)
    term = synthesise(
        jnp.concatenate(adjoint_re, 0),
        jnp.concatenate(adjoint_im, 0),
        phase[...],
        inverse_x[...],
        parts(plane),
    )
    for i in range(C):
        total = term[i]
        for o in range(C):
            total = total + (point[i, o] * 0.5) * up[o]
        cells[i] = total
        send(cells.at[i], grad_fields.at[i])
    for copy in copies:
        copy.wait()


def position_phase():
    shape = (2, MODES)
    lane = lax.broadcasted_iota(jnp.int32, shape, 1)
    steps = (lane // K) * lax.axis_index("row") + (lane % K) * lax.axis_index("col")
    angle = (steps % K).astype(jnp.float32) * (2.0 * math.pi / K)
    row = lax.broadcasted_iota(jnp.int32, shape, 0)
    return jnp.where(row == 0, jnp.cos(angle), -jnp.sin(angle))


def near(value):
    return pltpu.with_memory_space_constraint(value, pltpu.VMEM)


def far(value):
    return pltpu.with_memory_space_constraint(value, pltpu.HBM)


def near_out(shape, dtype=jnp.float32):
    return pltpu.VMEM(shape, dtype)


def groups():
    index = np.arange(256).reshape(2, 8, 4, 2, 2)
    index[0] = index[0, :, :, ::-1]
    index = index[::-1, [4, 5, 3, 6, 2, 7, 1, 0]][:, :, [2, 3, 1, 0], :, ::-1]
    index = index.reshape(K, K)
    return index.tolist(), index.T.tolist()


def swap(pieces, members):
    return lax.all_to_all(
        pieces, ("row", "col"), 0, 0, tiled=True, axis_index_groups=members
    )


def call(kernel, out_shape, in_specs, scratch_shapes=(), **more):
    where = [VMEM if not isinstance(o, jax.ShapeDtypeStruct) else HBM for o in out_shape]
    return pl.pallas_call(
        kernel,
        out_shape=tuple(out_shape),
        in_specs=in_specs,
        out_specs=tuple(where),
        scratch_shapes=scratch_shapes,
        compiler_params=PARAMS,
        **more,
    )


def total_modes(partial, *beside):
    shape = (K, 2 * C, MODES)
    near_by, alike = groups()
    pieces = near(swap(partial, near_by))
    (pieces,) = call(spread_kernel, [near_out(shape)], [VMEM])(pieces)
    pieces, *beside = lax.optimization_barrier((swap(pieces, alike), *beside))
    pieces = near(pieces)
    (pieces,) = call(spread_kernel, [near_out(shape)], [VMEM])(pieces)
    return near(swap(pieces, near_by)), *beside


def per_device(fields, cotangent, spec_weights, point_weights, bias):
    forward_x, scaled_x, inverse_x, plane = [jnp.asarray(t) for t in tables()]
    shape = fields.shape
    cells = (C, CELLS, N)
    partial, fields, forward_x, plane, phase = call(
        analysis_kernel,
        [
            near_out((K, 2 * C, MODES)),
            near_out(cells),
            near_out(forward_x.shape, jnp.bfloat16),
            near_out(plane.shape, jnp.bfloat16),
            near_out((2, MODES)),
        ],
        [HBM] * 3,
        [pltpu.SemaphoreType.DMA((C + 2,))],
    )(far(fields.reshape(cells)), far(forward_x), far(plane))
    partial, cotangent = lax.optimization_barrier((partial, cotangent))
    fields, cotangent, forward_x, scaled_x, inverse_x, plane, phase = [
        near(v)
        for v in (
            fields, cotangent.reshape(cells), forward_x, scaled_x, inverse_x, plane, phase
        )
    ]
    weights = spec_weights.reshape(2, C, C, K, MODES)
    (local,) = call(
        local_kernel, [near_out(cells)], [VMEM] + [SMEM] * 2, input_output_aliases={0: 0}
    )(fields, point_weights, bias)
    modes, weights, local = total_modes(partial, weights, local)
    weights = near(weights)
    upstream, partial = call(
        forward_kernel,
        [near_out(cells), near_out((K, 2 * C, MODES))],
        [VMEM] * 8,
    )(modes, weights, near(local), cotangent, phase, forward_x, scaled_x, plane)
    (back,) = total_modes(partial)
    grad_fields, grad_spectral = call(
        backward_kernel,
        [
            jax.ShapeDtypeStruct(cells, jnp.float32),
            jax.ShapeDtypeStruct((2, C, C, K, K, K), jnp.float32),
        ],
        [VMEM] * 4 + [SMEM] + [VMEM] * 3,
        [
            pltpu.VMEM(cells, jnp.float32),
            pltpu.VMEM((2, C, C, K, K, K), jnp.float32),
            pltpu.SemaphoreType.DMA((12,)),
        ],
    )(modes, back, weights, near(upstream), point_weights, phase, inverse_x, plane)
    return grad_fields.reshape(shape), grad_spectral


def solution(mesh):
    placed = P(None, None, "row", "col", None)
    return jax.shard_map(
        per_device,
        mesh=mesh,
        in_specs=(placed, placed, P(), P(), P()),
        out_specs=(placed, P()),
        check_vma=False,
    )
```

```python
import functools
import math

import jax
import jax.numpy as jnp
import numpy as np
from jax import lax
from jax.experimental import pallas as pl
from jax.experimental.pallas import tpu as pltpu
from jax.sharding import PartitionSpec as P

C = 4
N = 256
K = 16
LOCAL = 16
CELLS = LOCAL * LOCAL
MODES = K * K
ROWS = 2 * C * K
HALF_ROOT = math.sqrt(0.5)

VMEM = pl.BlockSpec(memory_space=pltpu.VMEM)
HBM = pl.BlockSpec(memory_space=pltpu.HBM)
SMEM = pl.BlockSpec(memory_space=pltpu.SMEM)
PARAMS = pltpu.CompilerParams(vmem_limit_bytes=24 << 20)
NT = (((1,), (1,)), ((), ()))
NN = (((1,), (0,)), ((), ()))
TN = (((0,), (0,)), ((), ()))


def two_parts(table):
    high = np.asarray(table, jnp.bfloat16)
    low = np.asarray(table - np.asarray(high, np.float64), jnp.bfloat16)
    return np.stack([high, low])


def joined(table):
    high, low = two_parts(table)
    return np.concatenate([high, high, low], 0)


def signed_waves():
    index = np.arange(K)
    return np.where(index < K // 2, index, index - K)


def tables():
    angle = 2.0 * np.pi / N * (np.arange(K)[:, None] * np.arange(N)[None, :] % N)
    forward_x = np.concatenate([np.cos(angle), -np.sin(angle)], 0)
    weighting = np.where(np.arange(K) == 0, 1.0, 2.0)[:, None] / float(N) ** 3
    inverse_x = np.concatenate([np.cos(angle) * weighting, -np.sin(angle) * weighting], 0)
    one = np.arange(LOCAL)[:, None] * signed_waves()[None, :]
    both = one[:, None, :, None] + one[None, :, None, :]
    angle = 2.0 * np.pi / N * (both.reshape(CELLS, MODES) % N)
    plane = np.concatenate([np.cos(angle), -np.sin(angle)], 1)
    scaled_x, inverse_x = joined(inverse_x * np.sqrt(0.5)), joined(inverse_x * 0.5)
    return two_parts(forward_x), scaled_x, inverse_x, two_parts(plane)


def split(value):
    high = value.astype(jnp.bfloat16)
    low = (value - high.astype(jnp.float32)).astype(jnp.bfloat16)
    return high, low


def dot_of(dims):
    return functools.partial(
        lax.dot_general, dimension_numbers=dims, preferred_element_type=jnp.float32
    )


def dot3(left, right, dims):
    dot = dot_of(dims)
    rows = left[0].shape[0]
    both = dot(jnp.concatenate(left, 0), right[0])
    return both[:rows] + (dot(left[0], right[1]) + both[rows:])


def analyse(channel, phase, forward_x, plane, out, ready=None):
    real, imag = [], []
    for c in range(C):
        along_x = dot3(forward_x, split(channel(c)), NT)
        real.append(along_x[:K])
        imag.append(along_x[K:])
    if ready is not None:
        ready()
    both = dot3(split(jnp.concatenate(real + imag, 0)), parts(plane), NN)
    half = ROWS // 2
    part_re = both[:half, :MODES] - both[half:, MODES:]
    part_im = both[:half, MODES:] + both[half:, :MODES]
    cosine, sine = phase[0:1, :], phase[1:2, :]
    for t, part in enumerate(
        (part_re * cosine - part_im * sine, part_re * sine + part_im * cosine)
    ):
        for c in range(C):
            out[:, t * C + c, :] = part[c * K : (c + 1) * K]


def synthesise(modes_re, modes_im, phase, inverse_x, plane):
    cosine, sine = phase[0:1, :], phase[1:2, :]
    here_re = modes_re * cosine + modes_im * sine
    here_im = modes_im * cosine - modes_re * sine
    left = jnp.concatenate(
        [jnp.concatenate([here_re, here_im], 1), jnp.concatenate([here_im, -here_re], 1)], 0
    )
    lines = dot3(split(left), plane, NT)
    half = ROWS // 2
    out = []
    for c in range(C):
        pair = jnp.concatenate([lines[c * K : (c + 1) * K], lines[half + c * K :][:K]], 0)
        high, low = split(pair)
        out.append(dot_of(TN)(jnp.concatenate([high, low, high], 0), inverse_x))
    return out


def parts(ref):
    return ref[0], ref[1]


def analysis_kernel(fields, forward_x, plane, out, cells, lines, square, phase, arrived):
    table = pltpu.make_async_copy(forward_x, lines, arrived.at[C])
    table.start()
    copies = [
        pltpu.make_async_copy(fields.at[c], cells.at[c], arrived.at[c]) for c in range(C)
    ]
    for copy in copies:
        copy.start()
    second = pltpu.make_async_copy(plane, square, arrived.at[C + 1])
    second.start()
    phase[...] = position_phase()
    table.wait()

    def channel(c):
        if c % 2 == 0:
            copies[c].wait()
            copies[c + 1].wait()
        return cells[c]

    analyse(channel, phase[...], parts(lines), square, out, second.wait)


def spread_kernel(pieces, out):
    total = jnp.sum(pieces[...], axis=0)
    out[...] = jnp.broadcast_to(total[None], out.shape)


def local_kernel(fields, point, bias, out):
    del fields
    for start in range(0, CELLS, 8):
        cells = [out[i, start : start + 8] for i in range(C)]
        for o in range(C):
            total = bias[o] * HALF_ROOT
            for i in range(C):
                total = total + (point[i, o] * HALF_ROOT) * cells[i]
            out[o, start : start + 8] = total


def forward_kernel(
    modes, weights, local, cotangent, phase, forward_x, scaled_x, plane, up, out
):
    mixed_re, mixed_im = [], []
    for o in range(C):
        re = im = 0.0
        for i in range(C):
            a, b = modes[:, i, :], modes[:, C + i, :]
            w, v = weights[0, i, o], weights[1, i, o]
            re = re + (a * w - b * v)
            im = im + (a * v + b * w)
        mixed_re.append(re)
        mixed_im.append(im)
    term = synthesise(
        jnp.concatenate(mixed_re, 0),
        jnp.concatenate(mixed_im, 0),
        phase[...],
        scaled_x[...],
        parts(plane),
    )
    for o in range(C):
        s = term[o] + local[o]
        bell = jnp.exp2(s * s * (-1.0 / math.log(2.0)))
        up[o] = cotangent[o] * ((1.0 + lax.erf(s)) + s * (2.0 / math.sqrt(math.pi)) * bell)
    analyse(lambda c: up[c], phase[...], parts(forward_x), plane, out)


def turned(modes):
    shape = (MODES, MODES)
    source, target = [lax.broadcasted_iota(jnp.int32, shape, axis) for axis in range(2)]
    wanted = target // 128 * 128 + (8 - target % 128 // K) % 8 * K + target % K
    order = (source == wanted).astype(jnp.bfloat16)
    high, rest = split_off(modes.reshape(ROWS, MODES))
    middle, rest = split_off(rest)
    total = 0.0
    for part in (rest.astype(jnp.bfloat16), middle, high):
        total = total + jnp.dot(part, order, preferred_element_type=jnp.float32)
    return total


def split_off(value):
    high = value.astype(jnp.bfloat16)
    return high, value - high.astype(jnp.float32)


def slabs(rows, start):
    half = rows[:, start : start + 128]
    return [
        pltpu.roll(jnp.broadcast_to(half[k : k + 1], (8, 128)), 0, 1, stride=K, stride_axis=0)
        for k in range(2 * C)
    ]


def backward_kernel(
    modes,
    back,
    weights,
    up,
    point,
    phase,
    inverse_x,
    plane,
    grad_fields,
    grad_spectral,
    cells,
    stored,
    sent,
):
    copies = []

    def send(source, target):
        copies.append(pltpu.make_async_copy(source, target, sent.at[len(copies)]))
        copies[-1].start()

    def one_wave(p):
        factor = (0.5 if p == 0 else 1.0) / float(N) ** 3
        first, second = [v[p * 2 * C : (p + 1) * 2 * C] for v in (modes_turned, back_turned)]
        second = second * factor
        for half in range(2):
            u, h = slabs(first, half * 128), slabs(second, half * 128)
            for i in range(C):
                for o in range(C):
                    re = u[i] * h[o] + u[C + i] * h[C + o]
                    im = u[i] * h[C + o] - u[C + i] * h[o]
                    stored[0, i, o, p, half * 8 : half * 8 + 8, :] = re[:, :K]
                    stored[1, i, o, p, half * 8 : half * 8 + 8, :] = im[:, :K]

    modes_turned, back_turned = turned(modes[...]), turned(back[...])
    for p in range(K):
        one_wave(p)
        some = pl.ds(p, 1)
        send(stored.at[:, :, :, some], grad_spectral.at[:, :, :, some])
    adjoint_re, adjoint_im = [], []
    for i in range(C):
        re = im = 0.0
        for o in range(C):
            a, b = back[:, o, :], back[:, C + o, :]
            w, v = weights[0, i, o], weights[1, i, o]
            re = re + (a * w + b * v)
            im = im + (b * w - a * v)
        adjoint_re.append(re)
        adjoint_im.append(im)
    term = synthesise(
        jnp.concatenate(adjoint_re, 0),
        jnp.concatenate(adjoint_im, 0),
        phase[...],
        inverse_x[...],
        parts(plane),
    )
    for i in range(C):
        total = term[i]
        for o in range(C):
            total = total + (point[i, o] * 0.5) * up[o]
        cells[i] = total
        send(cells.at[i], grad_fields.at[i])
    for copy in copies:
        copy.wait()


def position_phase():
    shape = (2, MODES)
    lane = lax.broadcasted_iota(jnp.int32, shape, 1)
    steps = (lane // K) * lax.axis_index("row") + (lane % K) * lax.axis_index("col")
    angle = (steps % K).astype(jnp.float32) * (2.0 * math.pi / K)
    row = lax.broadcasted_iota(jnp.int32, shape, 0)
    return jnp.where(row == 0, jnp.cos(angle), -jnp.sin(angle))


def near(value):
    return pltpu.with_memory_space_constraint(value, pltpu.VMEM)


def far(value):
    return pltpu.with_memory_space_constraint(value, pltpu.HBM)


def near_out(shape, dtype=jnp.float32):
    return pltpu.VMEM(shape, dtype)


def groups():
    index = np.arange(256).reshape(2, 8, 4, 2, 2)
    index[0] = index[0, :, :, ::-1]
    index = index[::-1, [4, 5, 3, 6, 2, 7, 1, 0]][:, :, [2, 3, 1, 0], :, ::-1]
    index = index.reshape(K, K)
    return index.tolist(), index.T.tolist()


def swap(pieces, members):
    return lax.all_to_all(
        pieces, ("row", "col"), 0, 0, tiled=True, axis_index_groups=members
    )


def call(kernel, out_shape, in_specs, scratch_shapes=(), **more):
    where = [VMEM if not isinstance(o, jax.ShapeDtypeStruct) else HBM for o in out_shape]
    return pl.pallas_call(
        kernel,
        out_shape=tuple(out_shape),
        in_specs=in_specs,
        out_specs=tuple(where),
        scratch_shapes=scratch_shapes,
        compiler_params=PARAMS,
        **more,
    )


def total_modes(partial, *beside):
    shape = (K, 2 * C, MODES)
    near_by, alike = groups()
    pieces = near(swap(partial, near_by))
    (pieces,) = call(spread_kernel, [near_out(shape)], [VMEM])(pieces)
    pieces, *beside = lax.optimization_barrier((swap(pieces, alike), *beside))
    pieces = near(pieces)
    (pieces,) = call(spread_kernel, [near_out(shape)], [VMEM])(pieces)
    return near(swap(pieces, near_by)), *beside


def per_device(fields, cotangent, spec_weights, point_weights, bias):
    forward_x, scaled_x, inverse_x, plane = [jnp.asarray(t) for t in tables()]
    shape = fields.shape
    cells = (C, CELLS, N)
    partial, fields, forward_x, plane, phase = call(
        analysis_kernel,
        [
            near_out((K, 2 * C, MODES)),
            near_out(cells),
            near_out(forward_x.shape, jnp.bfloat16),
            near_out(plane.shape, jnp.bfloat16),
            near_out((2, MODES)),
        ],
        [HBM] * 3,
        [pltpu.SemaphoreType.DMA((C + 2,))],
    )(far(fields.reshape(cells)), far(forward_x), far(plane))
    partial, cotangent = lax.optimization_barrier((partial, cotangent))
    fields, cotangent, forward_x, scaled_x, inverse_x, plane, phase = [
        near(v)
        for v in (
            fields, cotangent.reshape(cells), forward_x, scaled_x, inverse_x, plane, phase
        )
    ]
    weights = spec_weights.reshape(2, C, C, K, MODES)
    (local,) = call(
        local_kernel, [near_out(cells)], [VMEM] + [SMEM] * 2, input_output_aliases={0: 0}
    )(fields, point_weights, bias)
    modes, weights, local = total_modes(partial, weights, local)
    weights = near(weights)
    upstream, partial = call(
        forward_kernel,
        [near_out(cells), near_out((K, 2 * C, MODES))],
        [VMEM] * 8,
    )(modes, weights, near(local), cotangent, phase, forward_x, scaled_x, plane)
    (back,) = total_modes(partial)
    grad_fields, grad_spectral = call(
        backward_kernel,
        [
            jax.ShapeDtypeStruct(cells, jnp.float32),
            jax.ShapeDtypeStruct((2, C, C, K, K, K), jnp.float32),
        ],
        [VMEM] * 4 + [SMEM] + [VMEM] * 3,
        [
            pltpu.VMEM(cells, jnp.float32),
            pltpu.VMEM((2, C, C, K, K, K), jnp.float32),
            pltpu.SemaphoreType.DMA((K + C,)),
        ],
    )(modes, back, weights, near(upstream), point_weights, phase, inverse_x, plane)
    return grad_fields.reshape(shape), grad_spectral


def solution(mesh):
    placed = P(None, None, "row", "col", None)
    return jax.shard_map(
        per_device,
        mesh=mesh,
        in_specs=(placed, placed, P(), P(), P()),
        out_specs=(placed, P()),
        check_vma=False,
    )
```
